32 devices in a mesh: groups: 2 (over y), fsdp: 4 (over z), tensor: 4 (over x, core).
Axes of the slice: x: 2, y: 2, z: 4, core: 2. Of those that a mesh axis runs over, the one named last changes fastest.
Arguments:
- tokens: bfloat16 [2048, 4608], P(('groups', 'fsdp'), 'tensor'), parts along dimension 0, may hold values from -100 to 100
- norm_gain: bfloat16 [4608], P('tensor'), may hold values from 0.25 to 1.75
- w_query: bfloat16 [4608, 4096], P('fsdp', 'tensor'), may hold values from -0.5 to 0.5
- w_key: bfloat16 [4608, 2048], P('fsdp', 'tensor'), may hold values from -0.09375 to 0.09375
- w_value: bfloat16 [4608, 2048], P('fsdp', 'tensor'), may hold values from -0.09375 to 0.09375
- w_out: bfloat16 [4096, 4608], P('tensor', 'fsdp'), may hold values from -0.5 to 0.5
- post_gain: bfloat16 [4608], P('tensor'), may hold values from 0.25 to 1.75
Outputs:
- mixed: float32 [2048, 4608], P(('groups', 'fsdp'), 'tensor'), parts along dimension 0
The draws below stay inside these ranges and needn't reach their ends.
There are 2 independent parts, one for each index of `groups`. The reference program is written for one: setup_inputs(seed, part) draws one part's arguments, and reference() takes and returns one part's arrays. A program takes and returns all parts, laid end to end along the dimension named above; an argument that names none is the same for every part. Nothing has to cross between parts.
All inputs are finite; a program needn't handle non-finite values.
Results may differ from the reference program's by a relative error of at most 0.0053.
Values may be sent and summed in bfloat16 or wider, within the bound.
A program may use at most 128 MiB of HBM per device.

```python
import jax
import jax.numpy as jnp
from jax import lax

D = 4608
HEAD_DIM = 128
HEADS = 32
KV_HEADS = 16
LEN = 256
TOKENS = 1024
BLOCK_COLS = 1024
N_TENSOR = 4


def draw_tokens(key, part):
    base_key, col_key, row_key = jax.random.split(key, 3)
    col = jnp.arange(D, dtype=jnp.float32) / D
    col_scale = 10.0 ** (col - 0.5 + 0.3 * jax.random.uniform(col_key, (D,), jnp.float32, -1.0, 1.0))
    row_scale = 10.0 ** jax.random.uniform(row_key, (TOKENS, 1), jnp.float32, -0.5, 0.5)
    base = jnp.clip(jax.random.normal(base_key, (TOKENS, D), jnp.float32), -5.0, 5.0)
    return (base * row_scale * col_scale[None, :]).astype(jnp.bfloat16)


def draw_w_out(key, part):
    base_key, col_key = jax.random.split(key, 2)
    rows = HEADS * HEAD_DIM
    col = jnp.arange(D, dtype=jnp.float32) / D
    col_scale = 10.0 ** (0.8 * col - 0.4 + 0.2 * jax.random.uniform(col_key, (D,), jnp.float32, -1.0, 1.0))
    base = jnp.clip(jax.random.normal(base_key, (rows, D), jnp.float32), -5.0, 5.0)
    return (base * col_scale[None, :] / jnp.sqrt(jnp.float32(rows))).astype(jnp.bfloat16)


def shard_levels(stream_key, dims, cuts, least, largest):
    def one(dim, blocks):
        heights = jax.random.uniform(jax.random.fold_in(jax.random.fold_in(stream_key, 6), dim), (blocks,), jnp.float32, least / len(cuts), largest / len(cuts))
        return jnp.repeat(jnp.exp(heights), dims[dim] // blocks).reshape((-1,) + (1,) * (len(dims) - dim - 1))

    factor_of = one(*cuts[0])
    for cut in cuts[1:]:
        factor_of = factor_of * one(*cut)
    return factor_of


def normal_values(rng, extent, spread, limit, shards=(), kind=jnp.bfloat16):
    level = shard_levels(rng, extent, shards, -0.22, 0.18) if shards else 1.0
    array = jax.random.normal(rng, extent, jnp.float32) * spread * level
    return jnp.minimum(jnp.maximum(array, -limit), limit).astype(kind)


def setup_inputs(seed: int = 0, part: int = 0) -> dict:
    streams_of = jax.random.split(jax.random.key(seed), 8)
    part_splits = jax.random.split(jax.random.fold_in(streams_of[7], part), 8)
    tokens = draw_tokens(jax.random.fold_in(jax.random.fold_in(streams_of[7], part), 71), part)
    norm_gain = jnp.clip(1.0 + 0.15 * jax.random.normal(streams_of[1], (D,), jnp.float32), 0.25, 1.75).astype(jnp.bfloat16)
    w_query = normal_values(streams_of[2], (D, HEADS * HEAD_DIM), (D // 36) ** -0.5, 0.5, ((0, 4), (1, 4)))
    w_key = normal_values(streams_of[3], (D, KV_HEADS * HEAD_DIM), D ** -0.5, 0.09375, ((0, 4), (1, 4)))
    w_value = normal_values(streams_of[4], (D, KV_HEADS * HEAD_DIM), D ** -0.5, 0.09375, ((0, 4), (1, 4)))
    w_out = draw_w_out(jax.random.fold_in(streams_of[7], 71), part)
    post_gain = jnp.clip(1.0 + 0.15 * jax.random.normal(streams_of[6], (D,), jnp.float32), 0.25, 1.75).astype(jnp.bfloat16)
    return {"tokens": tokens, "norm_gain": norm_gain, "w_query": w_query, "w_key": w_key, "w_value": w_value, "w_out": w_out, "post_gain": post_gain}


eps_norm = 1e-06
soft_cap = 50.0
attn_scale = 144.0 ** (-0.5)
rope_base = 10000.0

def rotate(values, position):
    head_dim = values.shape[-1]
    half = head_dim // 2
    freq = rope_base ** (-(jnp.arange(half, dtype=jnp.float32) * 2.0 / head_dim))
    angle = position.astype(jnp.float32)[:, None] * freq[None, :]
    cosine = jnp.cos(angle)[:, None, :]
    sine = jnp.sin(angle)[:, None, :]
    first = values[..., :half]
    second = values[..., half:]
    return jnp.concatenate([first * cosine - second * sine, second * cosine + first * sine], axis=-1)

def attend(query, keys, values):
    count, heads, head_dim = query.shape
    kv_count = keys.shape[1]
    grouped = query.reshape(count, kv_count, heads // kv_count, head_dim).astype(jnp.float32)
    scores = jnp.einsum('nkgd,mkd->kgnm', grouped, keys.astype(jnp.float32)) * attn_scale
    capped = soft_cap * jnp.tanh(scores / soft_cap)
    spots = jnp.arange(count)
    allowed = spots[None, :] <= spots[:, None]
    weights = jnp.where(allowed, jnp.exp(capped), 0.0)
    probs = (weights / lax.optimization_barrier(jnp.sum(weights, axis=-1, keepdims=True))).astype(jnp.bfloat16)
    mixed = jnp.einsum('kgnm,mkd->nkgd', probs.astype(jnp.float32), values.astype(jnp.float32))
    return mixed.reshape(count, heads * head_dim).astype(jnp.bfloat16)

def reference(tokens, norm_gain, w_query, w_key, w_value, w_out, post_gain):
    local = tokens.astype(jnp.float32)
    total = lax.optimization_barrier(jnp.sum(local * local, axis=1))
    normed = (local * lax.rsqrt(total / D + eps_norm)[:, None] * norm_gain.astype(jnp.float32)).astype(jnp.bfloat16)
    query_raw = jnp.dot(normed, w_query, preferred_element_type=jnp.float32)
    key_raw = jnp.dot(normed, w_key, preferred_element_type=jnp.float32)
    value_raw = jnp.dot(normed, w_value, preferred_element_type=jnp.float32)
    position = (jnp.arange(TOKENS) % LEN).astype(jnp.int32)
    query = rotate(query_raw.reshape(TOKENS, HEADS, HEAD_DIM), position).astype(jnp.bfloat16)
    key = rotate(key_raw.reshape(TOKENS, KV_HEADS, HEAD_DIM), position).astype(jnp.bfloat16)
    value = value_raw.astype(jnp.bfloat16).reshape(TOKENS, KV_HEADS, HEAD_DIM)
    seq_count = TOKENS // LEN
    attn = lax.map(lambda item: attend(item[0], item[1], item[2]), (query.reshape(seq_count, LEN, HEADS, HEAD_DIM), key.reshape(seq_count, LEN, KV_HEADS, HEAD_DIM), value.reshape(seq_count, LEN, KV_HEADS, HEAD_DIM)))
    attn = attn.reshape(TOKENS, HEADS * HEAD_DIM)
    block = BLOCK_COLS
    proj = jnp.zeros((TOKENS, D), jnp.float32)
    for group in range(N_TENSOR):
        partial_value = jnp.dot(attn[:, group * block:(group + 1) * block], w_out[group * block:(group + 1) * block], preferred_element_type=jnp.float32)
        rounded = lax.optimization_barrier(partial_value.astype(jnp.bfloat16))
        proj = proj + rounded.astype(jnp.float32)
    post_total = lax.optimization_barrier(jnp.sum(proj * proj, axis=1))
    branch = proj * lax.rsqrt(post_total / D + eps_norm)[:, None] * post_gain.astype(jnp.float32)
    return local + branch
```

```python
import functools

import jax
import numpy as np
import jax.numpy as jnp
from jax import lax
from jax.experimental import pallas as pl
from jax.experimental.pallas import tpu as pltpu
from jax.sharding import PartitionSpec as P

HEAD_DIM = 128

eps_norm = 1e-06
soft_cap = 50.0
attn_scale = 144.0 ** (-0.5)
rope_base = 10000.0


def rotate(values, position):
    head_dim = values.shape[-1]
    half = head_dim // 2
    freq = rope_base ** (-(jnp.arange(half, dtype=jnp.float32) * 2.0 / head_dim))
    angle = position.astype(jnp.float32)[:, None] * freq[None, :]
    cosine = jnp.cos(angle)[:, None, :]
    sine = jnp.sin(angle)[:, None, :]
    first = values[..., :half]
    second = values[..., half:]
    return jnp.concatenate(
        [first * cosine - second * sine, second * cosine + first * sine], axis=-1
    )


def attend(query, keys, values, position):
    count, heads, head_dim = query.shape
    kv_count = keys.shape[1]
    grouped = query.reshape(count, kv_count, heads // kv_count, head_dim)
    scores = (
        jnp.einsum("nkgd,mkd->kgnm", grouped, keys, preferred_element_type=jnp.float32) * attn_scale
    )
    capped = soft_cap * jnp.tanh(scores / soft_cap)
    allowed = position[None, :] <= position[:, None]
    weights = jnp.where(allowed, jnp.exp(capped), 0.0)
    probs = (weights / jnp.sum(weights, axis=-1, keepdims=True)).astype(jnp.bfloat16)
    mixed = jnp.einsum("kgnm,mkd->nkgd", probs, values, preferred_element_type=jnp.float32)
    return mixed.reshape(count, heads * head_dim).astype(jnp.bfloat16)


def swap_pairs(n_fsdp, n_tensor, turn):
    ratio = n_fsdp // n_tensor
    pairs = []
    for f in range(n_fsdp):
        for t in range(n_tensor):
            j = (f + turn) % ratio
            pairs.append((f * n_tensor + t, (t * ratio + j) * n_tensor + f // ratio))
    return pairs


def to_rows(block, n_fsdp, n_tensor):
    rows = block.shape[0]
    ratio = n_fsdp // n_tensor
    width = block.shape[1] // ratio
    f = lax.axis_index("fsdp")
    if ratio == 1:
        held = lax.ppermute(block, ("fsdp", "tensor"), swap_pairs(n_fsdp, n_tensor, 0))
    else:
        held = jnp.zeros((ratio, rows, width), block.dtype)
        for turn in range(ratio):
            piece = lax.dynamic_slice_in_dim(block, (f + turn) % ratio * width, width, 1)
            got = lax.ppermute(piece, ("fsdp", "tensor"), swap_pairs(n_fsdp, n_tensor, turn))
            held = lax.dynamic_update_index_in_dim(held, got, (f - turn) % ratio, 0)
        held = held.reshape(ratio * rows, width)
    return lax.all_gather(held, "tensor", axis=0, tiled=True)


def from_rows(summed, rows, n_fsdp, n_tensor):
    ratio = n_fsdp // n_tensor
    width = summed.shape[1]
    f = lax.axis_index("fsdp")
    back = lambda turn: [(b, a) for a, b in swap_pairs(n_fsdp, n_tensor, turn)]
    if ratio == 1:
        return lax.ppermute(summed, ("fsdp", "tensor"), back(0))
    pieces = summed.reshape(ratio, rows, width)
    out = jnp.zeros((rows, ratio * width), summed.dtype)
    for turn in range(ratio):
        piece = lax.dynamic_index_in_dim(pieces, (f - turn) % ratio, 0, keepdims=False)
        got = lax.ppermute(piece, ("fsdp", "tensor"), back(turn))
        out = lax.dynamic_update_slice_in_dim(out, got, (f + turn) % ratio * width, 1)
    return out


MESH = pl.DeviceIdType.MESH
VMEM_LIMIT = 60 * 1024 * 1024
CHAIN = 4
LAG = 2
GATHER_AT = 15


def remote(src, dst, send, recv, a, b):
    return pltpu.make_async_remote_copy(
        src_ref=src,
        dst_ref=dst,
        send_sem=send,
        recv_sem=recv,
        device_id={"fsdp": a, "tensor": b},
        device_id_type=MESH,
    )


def greet(n, f, t):
    barrier = pltpu.get_barrier_semaphore()
    for a in range(n):
        for b in range(n):
            @pl.when(jnp.logical_not((f == a) & (t == b)))
            def _():
                pl.semaphore_signal(
                    barrier, inc=1, device_id={"fsdp": a, "tensor": b}, device_id_type=MESH
                )
    return lambda: pl.semaphore_wait(barrier, n * n - 1)


def loop(low, high, body):
    def step(i, carry):
        body(i)
        return carry

    lax.fori_loop(low, high, step, 0)


def row_sums(squares):
    groups = squares.shape[1] // 128
    lanes = squares[:, :128]
    for i in range(1, groups):
        lanes = lanes + squares[:, i * 128 : (i + 1) * 128]
    row = jnp.sum(lanes.T, axis=0, keepdims=True)
    return jnp.broadcast_to(row, (8, squares.shape[0]))


def as_column(row):
    return jnp.broadcast_to(row[:1], (128, row.shape[1])).T


def block_kernel(
    n, tok_ref, gains_ref, cos_ref, sin_ref, wq_hbm, wk_hbm, wv_hbm, wo_hbm, out_ref,
    w_all, wo, xn, xs, relay_buf, ss_mine, ss_got,
    near_stage, far_stage, near_got, far_got, keys, values, att,
    part_stage, part_got, pair_stage, pair_got, sum_stage, proj, post_mine, post_got,
    w_sem, ss_send, ss_recv, src_send, relay_recv, relay_send,
    x_recv, mate_send, cross_send, near_send, near_recv, far_send, far_recv,
    att_send, att_recv, part_send, part_recv, pair_send, pair_recv, sum_send, sum_recv,
    post_send, post_recv,
):
    f, t = lax.axis_index("fsdp"), lax.axis_index("tensor")
    rows, width = tok_ref.shape
    half = rows // 2
    kv = w_all.shape[0]
    per = att.shape[3] // HEAD_DIM
    count = 4 * kv
    lanes = width // 128
    total_width = width * n
    finish_greeting = greet(n, f, t)

    upper = f // 2
    inward = f + 1 - 2 * upper
    outward = f - 1 + 2 * upper
    at_end = (f == 0) | (f == n - 1)
    in_middle = (f > 0) & (f < n - 1)
    plane, core = t // 2, t % 2
    mate = t + 1 - 2 * core
    cross = (t + n // 2) % n
    leads = core == f % 2
    owner = f == t

    def near(c):
        return c + upper * (n - 1 - 2 * c)

    def far(c):
        return n - 1 - c + upper * (2 * c - n + 1)

    def rows_at(start, size):
        return pl.ds(start if isinstance(start, int) else pl.multiple_of(start, size), size)

    def side(h):
        return rows_at(h * half, half)

    fetches = []
    for g in range(kv):
        for ref, first, size in (
            (wq_hbm, 0, per * HEAD_DIM),
            (wk_hbm, per * HEAD_DIM, HEAD_DIM),
            (wv_hbm, (per + 1) * HEAD_DIM, HEAD_DIM),
        ):
            fetches.append(
                pltpu.make_async_copy(
                    ref.at[:, pl.ds(g * size, size)],
                    w_all.at[g, :, pl.ds(first, size)],
                    w_sem.at[len(fetches)],
                )
            )
    fetches.append(pltpu.make_async_copy(wo_hbm, wo, w_sem.at[len(fetches)]))
    for fetch in fetches:
        fetch.start()

    tok = tok_ref[...].astype(jnp.float32)
    ss_mine[...] = row_sums(tok * tok)
    finish_greeting()

    def total_out(k, slot):
        return remote(
            ss_mine, ss_got.at[slot], ss_send.at[k - 1], ss_recv.at[slot], f, (t + k) % n
        )

    for k in range(1, n):
        total_out(k, t).start()
    total = ss_mine[...]
    for k in range(1, n):
        slot = (t + k) % n
        total_out(k, slot).wait_recv()
        total = total + ss_got[slot]
    scale = lax.rsqrt(as_column(total) / total_width + eps_norm)
    for i in range(lanes):
        cols = slice(i * 128, (i + 1) * 128)
        xn[:, cols] = (
            tok_ref[:, cols].astype(jnp.float32) * scale * gains_ref[0:1, cols]
        ).astype(jnp.bfloat16)

    @pl.when(owner)
    def _():
        xs[f] = xn[...]

    def direct():
        return remote(
            xn.at[side(plane)], xs.at[f, side(plane)],
            src_send.at[0], x_recv.at[f, plane], t, t,
        )

    def to_relay():
        return remote(
            xn.at[side(1 - plane)], relay_buf, src_send.at[1], relay_recv, f, cross
        )

    def relayed():
        return remote(
            relay_buf, xs.at[f, side(plane)], relay_send, x_recv.at[f, plane], cross, t
        )

    def to_mate(r, h):
        return remote(
            xs.at[r, side(h)], xs.at[r, side(h)], mate_send.at[r, h], x_recv.at[r, h], f, mate
        )

    def to_cross(r, h):
        return remote(
            xs.at[r, side(h)], xs.at[r, side(h)], cross_send.at[r, h], x_recv.at[r, h], f, cross
        )

    @pl.when(jnp.logical_not(owner))
    def _():
        to_relay().start()
        direct().start()

    @pl.when(owner)
    def _():
        for h in range(2):
            to_cross(f, h).start()
            to_mate(f, h).start()

    @pl.when(cross != f)
    def _():
        to_relay().wait_recv()
        relayed().start()

    def spread(r):
        @pl.when(leads)
        def _():
            @pl.when(r != f)
            def _():
                to_mate(r, plane).wait_recv()
                to_cross(r, plane).start()
                to_mate(r, plane).start()
                to_mate(r, 1 - plane).wait_recv()
                to_mate(r, 1 - plane).start()

            @pl.when((r == f) & jnp.logical_not(owner))
            def _():
                for h in range(2):
                    to_mate(r, h).wait_recv()
                    to_mate(r, h).start()

        @pl.when(jnp.logical_not(leads))
        def _():
            for h in range(2):
                to_mate(r, h).wait_recv()

    def place(k):
        j = k // kv
        return j // 2, j % 2, k % kv

    def partial(seq, h, g):
        return jnp.dot(xs[seq, side(h)], w_all[g], preferred_element_type=jnp.float32)

    def near_hop(k, recv):
        landing = near_got if recv is near_recv else far_got
        return remote(
            near_stage.at[k], landing.at[k], near_send.at[k], recv.at[k], inward, t
        )

    def far_hop(k):
        return remote(
            far_stage.at[k], far_got.at[k], far_send.at[k], far_recv.at[k], outward, t
        )

    def first_near(k):
        c, h, g = place(k)
        near_stage[k] = partial(near(c), h, g).astype(jnp.bfloat16)
        near_hop(k, near_recv).start()

    def middle_near(k):
        c, h, g = place(k)
        part = partial(near(c), h, g)
        near_hop(k, near_recv).wait_recv()
        near_stage[k] = (part + near_got[k].astype(jnp.float32)).astype(jnp.bfloat16)
        near_hop(k, far_recv).start()

    def middle_far(k):
        c, h, g = place(k)
        part = partial(far(c), h, g)
        far_hop(k).wait_recv()
        far_stage[k] = (part + far_got[k].astype(jnp.float32)).astype(jnp.bfloat16)
        far_hop(k).start()

    def share(s, h, g, there):
        return remote(
            att.at[s, g, side(h)], att.at[s, g, side(h)],
            att_send.at[s, h, g], att_recv.at[s, h, g], there, t,
        )

    def turn(u, span):
        other = pltpu.roll(u, HEAD_DIM // 2, 1)
        return (u * cos_ref[span] + other * sin_ref[span]).astype(jnp.bfloat16)

    def attend_piece(c, h, g):
        k = (c * 2 + h) * kv + g
        span, seen = slice(h * half, (h + 1) * half), (h + 1) * half
        part = partial(far(c), h, g)
        far_hop(k).wait_recv()
        raw = part + far_got[k].astype(jnp.float32)
        heads = [raw[:, i * HEAD_DIM : (i + 1) * HEAD_DIM] for i in range(per + 2)]
        keys[c, g, span] = turn(heads[per], span)
        values[c, g, span] = heads[per + 1].astype(jnp.bfloat16)
        query = jnp.concatenate([turn(u, span) for u in heads[:per]], axis=0)
        scores = lax.dot_general(
            query, keys[c, g, :seen], (((1,), (1,)), ((), ())),
            preferred_element_type=jnp.float32,
        )
        capped = soft_cap * jnp.tanh(scores * (attn_scale / soft_cap))
        index = lax.broadcasted_iota(jnp.int32, (half, seen), 0) + h * half
        allowed = lax.broadcasted_iota(jnp.int32, (half, seen), 1) <= index
        allowed = jnp.concatenate([allowed] * per, axis=0)
        e = jnp.where(allowed, jnp.exp(capped), 0.0)
        inverse = 1.0 / jnp.sum(e, axis=1, keepdims=True)
        probs = (e * inverse).astype(jnp.bfloat16)
        mixed = jnp.dot(probs, values[c, g, :seen], preferred_element_type=jnp.float32)
        for i in range(per):
            att[far(c), g, span, i * HEAD_DIM : (i + 1) * HEAD_DIM] = mixed[
                i * half : (i + 1) * half
            ].astype(jnp.bfloat16)
        share(far(c), h, g, inward).start()

    quarter, eighth = half // 2, half // 4

    def part_hop(s, h):
        m = 2 * s + h
        return remote(
            part_stage.at[m, rows_at((1 - core) * quarter, quarter)], part_got.at[m],
            part_send.at[m], part_recv.at[m], f, mate,
        )

    def pair_hop(s, h):
        m = 2 * s + h
        return remote(
            pair_stage.at[m], pair_got.at[m], pair_send.at[m], pair_recv.at[m], f, cross
        )

    def sum_hop(s, h):
        m = 2 * s + h
        piece = core * 2 + plane
        return remote(
            sum_stage.at[m], proj.at[rows_at(h * half + piece * eighth, eighth)],
            sum_send.at[m], sum_recv.at[h, piece], s, f,
        )

    def pair_sum(m, which):
        kept = part_stage[m, rows_at(core * quarter + which * eighth, eighth)]
        got = part_got[m, rows_at(which * eighth, eighth)]
        return kept.astype(jnp.float32) + got.astype(jnp.float32)

    def out_first(s, h):
        m = 2 * s + h
        acc = jnp.dot(att[s, 0, side(h)], wo[: per * HEAD_DIM], preferred_element_type=jnp.float32)
        for g in range(1, kv):
            acc = acc + jnp.dot(
                att[s, g, side(h)],
                wo[g * per * HEAD_DIM : (g + 1) * per * HEAD_DIM],
                preferred_element_type=jnp.float32,
            )
        part_stage[m] = acc.astype(jnp.bfloat16)
        part_hop(s, h).start()

    def out_second(s, h):
        m = 2 * s + h
        part_hop(s, h).wait_recv()
        pair_stage[m] = pair_sum(m, 1 - plane).astype(jnp.bfloat16)
        pair_hop(s, h).start()

    def out_third(s, h):
        m = 2 * s + h
        pair_hop(s, h).wait_recv()
        summed = pair_sum(m, plane) + pair_got[m].astype(jnp.float32)
        stays = (s == f) & owner

        @pl.when(stays)
        def _():
            start = h * half + (core * 2 + plane) * eighth
            proj[rows_at(start, eighth)] = summed.astype(jnp.bfloat16)

        @pl.when(jnp.logical_not(stays))
        def _():
            sum_stage[m] = summed.astype(jnp.bfloat16)
            sum_hop(s, h).start()

    def advance(i, where):
        out_first(*where(i))
        pl.when(i >= 1)(lambda: out_second(*where(i - 1)))
        pl.when(i >= 2)(lambda: out_third(*where(i - 2)))

    def flush(where):
        out_second(*where(2 * n - 1))
        out_third(*where(2 * n - 2))
        out_third(*where(2 * n - 1))

    @pl.when(at_end)
    def _():
        def where(i):
            j = i % n
            c = j // 2
            return jnp.where(i < n, far(c), near(c)), j % 2

        spread(near(0))
        for fetch in fetches[:-1]:
            fetch.wait()
        loop(0, count // 2, first_near)
        spread(near(1))
        loop(count // 2, count, first_near)
        fetches[-1].wait()
        spread(far(0))
        spread(far(1))

        def chunk(c):
            for h in range(2):
                loop(0, kv, lambda g: attend_piece(c, h, g))
                advance(2 * c + h, where)

        loop(0, 2, chunk)

        def gather(i):
            s, h = where(i)
            for g in range(kv):
                share(s, h, g, inward).wait_recv()
            advance(i, where)

        loop(n, 2 * n, gather)
        flush(where)

    @pl.when(in_middle)
    def _():
        def where(i):
            j = i // 2
            c = j // 2
            return jnp.where(i % 2 == 0, far(c), near(c)), j % 2

        for r in (near(1), near(0), far(1), far(0)):
            spread(r)
        for fetch in fetches:
            fetch.wait()

        def pass_on(m, seq, there):
            for k in (2 * m, 2 * m + 1):
                c, h, g = place(k)
                share(seq(c), h, g, there).wait_recv()
                share(seq(c), h, g, there).start()

        def step(s):
            pl.when(s < count)(lambda: middle_near(s))
            pl.when((s >= LAG) & (s < count + LAG))(lambda: middle_far(s - LAG))
            m = s - GATHER_AT
            pl.when((m >= 0) & (m < count // 2))(lambda: pass_on(m, far, inward))
            pl.when((m >= 1) & (m < count // 2 + 1))(lambda: pass_on(m - 1, near, outward))
            pl.when(m >= 1)(lambda: advance(m - 1, where))

        loop(0, GATHER_AT + 2 * n + 1, step)
        flush(where)

    def post_out(h, k, slot):
        return remote(
            post_mine.at[h], post_got.at[h, slot],
            post_send.at[h, k - 1], post_recv.at[h, slot], f, (t + k) % n,
        )

    for h in range(2):
        for piece in range(n):
            mine = owner & (core * 2 + plane == piece)

            @pl.when(jnp.logical_not(mine))
            def _():
                spot = proj.at[rows_at(h * half + piece * eighth, eighth)]
                remote(
                    spot, spot, sum_send.at[0], sum_recv.at[h, piece], f, t
                ).wait_recv()

        branch = proj[side(h)].astype(jnp.float32)
        post_mine[h] = row_sums(branch * branch)
        for k in range(1, n):
            post_out(h, k, t).start()
    for h in range(2):
        total = post_mine[h]
        for k in range(1, n):
            slot = (t + k) % n
            post_out(h, k, slot).wait_recv()
            total = total + post_got[h, slot]
        scale = lax.rsqrt(as_column(total) / total_width + eps_norm)
        for i in range(lanes):
            cols = slice(i * 128, (i + 1) * 128)
            out_ref[side(h), cols] = tok_ref[side(h), cols].astype(jnp.float32) + (
                proj[side(h), cols].astype(jnp.float32) * scale * gains_ref[1:2, cols]
            )

    for k in range(1, n):
        total_out(k, t).wait_send()
        for h in range(2):
            post_out(h, k, t).wait_send()

    @pl.when(jnp.logical_not(owner))
    def _():
        to_relay().wait_send()
        direct().wait_send()

    pl.when(cross != f)(lambda: relayed().wait_send())

    def drain(r):
        @pl.when(leads)
        def _():
            for h in range(2):
                to_mate(r, h).wait_send()
                pl.when(((r != f) & (h == plane)) | ((r == f) & owner))(
                    lambda: to_cross(r, h).wait_send()
                )

        for h in range(2):
            part_hop(r, h).wait_send()
            pair_hop(r, h).wait_send()
            pl.when(jnp.logical_not((r == f) & owner))(lambda: sum_hop(r, h).wait_send())
            sent = in_middle | (r == far(0)) | (r == far(1))

            @pl.when(sent)
            def _():
                for g in range(kv):
                    share(r, h, g, inward).wait_send()

    loop(0, n, drain)

    def drain_hops(k):
        near_hop(k, far_recv).wait_send()
        pl.when(in_middle)(lambda: far_hop(k).wait_send())

    loop(0, count, drain_hops)


def whole_block(n, tokens, gains, cosine, sine, w_query, w_key, w_value, w_out):
    rows, width = tokens.shape
    half, kv = rows // 2, w_key.shape[1] // HEAD_DIM
    per = w_query.shape[1] // w_key.shape[1]
    wide = (per + 2) * HEAD_DIM
    count = 4 * kv
    dma = pltpu.SemaphoreType.DMA
    bf16 = lambda *shape: pltpu.VMEM(shape, jnp.bfloat16)
    f32 = lambda *shape: pltpu.VMEM(shape, jnp.float32)
    vmem = pl.BlockSpec(memory_space=pltpu.VMEM)
    anywhere = pl.BlockSpec(memory_space=pl.ANY)
    return pl.pallas_call(
        functools.partial(block_kernel, n),
        out_shape=jax.ShapeDtypeStruct((rows, width), jnp.float32),
        in_specs=[vmem] * 4 + [anywhere] * 4,
        out_specs=vmem,
        scratch_shapes=[
            bf16(kv, width, wide), bf16(*w_out.shape), bf16(rows, width),
            bf16(n, rows, width), bf16(half, width), f32(8, rows), f32(n, 8, rows),
            bf16(count, half, wide), bf16(count, half, wide),
            bf16(count, half, wide), bf16(count, half, wide),
            bf16(2, kv, rows, HEAD_DIM), bf16(2, kv, rows, HEAD_DIM),
            bf16(n, kv, rows, per * HEAD_DIM),
            bf16(2 * n, half, width), bf16(2 * n, half // 2, width),
            bf16(2 * n, half // 4, width), bf16(2 * n, half // 4, width),
            bf16(2 * n, half // 4, width), bf16(rows, width),
            f32(2, 8, half), f32(2, n, 8, half),
            dma((3 * kv + 1,)), dma((n - 1,)), dma((n,)), dma((2,)), dma(()), dma(()),
            dma((n, 2)), dma((n, 2)), dma((n, 2)),
            dma((count,)), dma((count,)), dma((count,)), dma((count,)),
            dma((n, 2, kv)), dma((n, 2, kv)),
            dma((2 * n,)), dma((2 * n,)), dma((2 * n,)), dma((2 * n,)),
            dma((2 * n,)), dma((2, n)),
            dma((2, n - 1)), dma((2, n)),
        ],
        compiler_params=pltpu.CompilerParams(
            collective_id=0, has_side_effects=True, vmem_limit_bytes=VMEM_LIMIT
        ),
    )(tokens, gains, cosine, sine, w_query, w_key, w_value, w_out)


def tables(rows):
    half = HEAD_DIM // 2
    freq = np.float32(rope_base) ** (-(np.arange(half, dtype=np.float32) * np.float32(2.0 / HEAD_DIM)))
    angle = np.arange(rows, dtype=np.float32)[:, None] * freq[None, :].astype(np.float32)
    cosine, sine = np.cos(angle), np.sin(angle)
    return (
        jnp.asarray(np.concatenate([cosine, cosine], axis=1), jnp.float32),
        jnp.asarray(np.concatenate([-sine, sine], axis=1), jnp.float32),
    )


def solution(mesh):
    n_fsdp, n_tensor = mesh.shape["fsdp"], mesh.shape["tensor"]

    def on_device(tokens, norm_gain, w_query, w_key, w_value, w_out, post_gain):
        rows = tokens.shape[0]
        width = tokens.shape[1] * n_tensor
        if n_fsdp == n_tensor == CHAIN:
            gains = jnp.stack([norm_gain, post_gain]).astype(jnp.float32)
            return whole_block(
                n_fsdp, tokens, gains, *tables(rows), w_query, w_key, w_value, w_out
            )
        widened = tokens.astype(jnp.float32)
        total = lax.psum(jnp.sum(widened * widened, axis=1), "tensor")
        normed = (
            widened * lax.rsqrt(total / width + eps_norm)[:, None] * norm_gain.astype(jnp.float32)
        ).astype(jnp.bfloat16)
        mine = to_rows(normed, n_fsdp, n_tensor)
        raw = []
        for piece in (w_query, w_key, w_value):
            part = jnp.dot(mine, piece, preferred_element_type=jnp.float32).astype(jnp.bfloat16)
            parts = lax.all_to_all(part, "fsdp", 0, 0, tiled=True)
            parts = parts.reshape(n_fsdp, rows, piece.shape[1])
            raw.append(jnp.sum(parts.astype(jnp.float32), axis=0))
        query_raw, key_raw, value_raw = raw
        position = jnp.arange(rows, dtype=jnp.int32)
        local_heads = w_query.shape[1] // HEAD_DIM
        local_kv = w_key.shape[1] // HEAD_DIM
        query = rotate(query_raw.reshape(rows, local_heads, HEAD_DIM), position)
        key = rotate(key_raw.reshape(rows, local_kv, HEAD_DIM), position)
        query, key = query.astype(jnp.bfloat16), key.astype(jnp.bfloat16)
        value = value_raw.astype(jnp.bfloat16).reshape(rows, local_kv, HEAD_DIM)
        attn = attend(query, key, value, position)
        attn_all = lax.all_gather(attn, "fsdp", axis=0, tiled=True)
        part = jnp.dot(attn_all, w_out, preferred_element_type=jnp.float32).astype(jnp.bfloat16)
        summed = lax.psum_scatter(part, "tensor", scatter_dimension=0, tiled=True)
        proj = from_rows(summed, rows, n_fsdp, n_tensor).astype(jnp.float32)
        post_total = lax.psum(jnp.sum(proj * proj, axis=1), "tensor")
        branch = (
            proj
            * lax.rsqrt(post_total / width + eps_norm)[:, None]
            * post_gain.astype(jnp.float32)
        )
        return tokens.astype(jnp.float32) + branch

    placed = (
        P(("groups", "fsdp"), "tensor"),
        P("tensor"),
        P("fsdp", "tensor"),
        P("fsdp", "tensor"),
        P("fsdp", "tensor"),
        P("tensor", "fsdp"),
        P("tensor"),
    )
    return jax.shard_map(
        on_device,
        mesh=mesh,
        in_specs=placed,
        out_specs=P(("groups", "fsdp"), "tensor"),
        check_vma=False,
    )
```

```python
import functools

import jax
import numpy as np
import jax.numpy as jnp
from jax import lax
from jax.experimental import pallas as pl
from jax.experimental.pallas import tpu as pltpu
from jax.sharding import PartitionSpec as P

HEAD_DIM = 128

eps_norm = 1e-06
soft_cap = 50.0
attn_scale = 144.0 ** (-0.5)
rope_base = 10000.0


def rotate(values, position):
    head_dim = values.shape[-1]
    half = head_dim // 2
    freq = rope_base ** (-(jnp.arange(half, dtype=jnp.float32) * 2.0 / head_dim))
    angle = position.astype(jnp.float32)[:, None] * freq[None, :]
    cosine = jnp.cos(angle)[:, None, :]
    sine = jnp.sin(angle)[:, None, :]
    first = values[..., :half]
    second = values[..., half:]
    return jnp.concatenate(
        [first * cosine - second * sine, second * cosine + first * sine], axis=-1
    )


def attend(query, keys, values, position):
    count, heads, head_dim = query.shape
    kv_count = keys.shape[1]
    grouped = query.reshape(count, kv_count, heads // kv_count, head_dim)
    scores = (
        jnp.einsum("nkgd,mkd->kgnm", grouped, keys, preferred_element_type=jnp.float32) * attn_scale
    )
    capped = soft_cap * jnp.tanh(scores / soft_cap)
    allowed = position[None, :] <= position[:, None]
    weights = jnp.where(allowed, jnp.exp(capped), 0.0)
    probs = (weights / jnp.sum(weights, axis=-1, keepdims=True)).astype(jnp.bfloat16)
    mixed = jnp.einsum("kgnm,mkd->nkgd", probs, values, preferred_element_type=jnp.float32)
    return mixed.reshape(count, heads * head_dim).astype(jnp.bfloat16)


def swap_pairs(n_fsdp, n_tensor, turn):
    ratio = n_fsdp // n_tensor
    pairs = []
    for f in range(n_fsdp):
        for t in range(n_tensor):
            j = (f + turn) % ratio
            pairs.append((f * n_tensor + t, (t * ratio + j) * n_tensor + f // ratio))
    return pairs


def to_rows(block, n_fsdp, n_tensor):
    rows = block.shape[0]
    ratio = n_fsdp // n_tensor
    width = block.shape[1] // ratio
    f = lax.axis_index("fsdp")
    if ratio == 1:
        held = lax.ppermute(block, ("fsdp", "tensor"), swap_pairs(n_fsdp, n_tensor, 0))
    else:
        held = jnp.zeros((ratio, rows, width), block.dtype)
        for turn in range(ratio):
            piece = lax.dynamic_slice_in_dim(block, (f + turn) % ratio * width, width, 1)
            got = lax.ppermute(piece, ("fsdp", "tensor"), swap_pairs(n_fsdp, n_tensor, turn))
            held = lax.dynamic_update_index_in_dim(held, got, (f - turn) % ratio, 0)
        held = held.reshape(ratio * rows, width)
    return lax.all_gather(held, "tensor", axis=0, tiled=True)


def from_rows(summed, rows, n_fsdp, n_tensor):
    ratio = n_fsdp // n_tensor
    width = summed.shape[1]
    f = lax.axis_index("fsdp")
    back = lambda turn: [(b, a) for a, b in swap_pairs(n_fsdp, n_tensor, turn)]
    if ratio == 1:
        return lax.ppermute(summed, ("fsdp", "tensor"), back(0))
    pieces = summed.reshape(ratio, rows, width)
    out = jnp.zeros((rows, ratio * width), summed.dtype)
    for turn in range(ratio):
        piece = lax.dynamic_index_in_dim(pieces, (f - turn) % ratio, 0, keepdims=False)
        got = lax.ppermute(piece, ("fsdp", "tensor"), back(turn))
        out = lax.dynamic_update_slice_in_dim(out, got, (f + turn) % ratio * width, 1)
    return out


MESH = pl.DeviceIdType.MESH
VMEM_LIMIT = 60 * 1024 * 1024
CHAIN = 4
LAG = 2
FAR_AT, FAR_PACE = 15, 2
NEAR_AT, NEAR_PACE = 17, 2
OUT_AT = 18
ENTRY, OTHER, LAST = 0, 1, 2


def remote(src, dst, send, recv, a, b):
    return pltpu.make_async_remote_copy(
        src_ref=src,
        dst_ref=dst,
        send_sem=send,
        recv_sem=recv,
        device_id={"fsdp": a, "tensor": b},
        device_id_type=MESH,
    )


def greet(n, f, t):
    barrier = pltpu.get_barrier_semaphore()
    for a in range(n):
        for b in range(n):
            @pl.when(jnp.logical_not((f == a) & (t == b)))
            def _():
                pl.semaphore_signal(
                    barrier, inc=1, device_id={"fsdp": a, "tensor": b}, device_id_type=MESH
                )
    return lambda: pl.semaphore_wait(barrier, n * n - 1)


def loop(low, high, body):
    def step(i, carry):
        body(i)
        return carry

    lax.fori_loop(low, high, step, 0)


def row_sums(squares):
    groups = squares.shape[1] // 128
    lanes = squares[:, :128]
    for i in range(1, groups):
        lanes = lanes + squares[:, i * 128 : (i + 1) * 128]
    row = jnp.sum(lanes.T, axis=0, keepdims=True)
    return jnp.broadcast_to(row, (8, squares.shape[0]))


def as_column(row):
    return jnp.broadcast_to(row[:1], (128, row.shape[1])).T


def block_kernel(
    n, tok_hbm, gain_hbm, post_hbm, cos_hbm, sin_hbm, wq_hbm, wk_hbm, wv_hbm, wo_hbm, out_ref,
    tok_ref, gain_ref, post_ref, cos_ref, sin_ref, small_sem, w_all, wo, xn, xs, relay_buf, ss_mine, ss_got,
    near_stage, far_stage, near_got, far_got, keys, values, att,
    part_stage, part_got, pair_stage, pair_got, sum_stage, proj, post_mine, post_got,
    w_sem, ss_send, ss_recv, src_send, relay_recv, relay_send,
    x_recv, mate_send, cross_send, near_send, near_recv, far_send, far_recv,
    att_send, att_recv, part_send, part_recv, pair_send, pair_recv, sum_send, sum_recv,
    post_send, post_recv,
):
    f, t = lax.axis_index("fsdp"), lax.axis_index("tensor")
    rows, width = tok_ref.shape
    half = rows // 2
    kv = w_all.shape[0]
    per = att.shape[3] // HEAD_DIM
    count = 4 * kv
    lanes = width // 128
    total_width = width * n
    finish_greeting = greet(n, f, t)

    upper = f // 2
    inward = f + 1 - 2 * upper
    outward = f - 1 + 2 * upper
    at_end = (f == 0) | (f == n - 1)
    in_middle = (f > 0) & (f < n - 1)
    plane, core = t // 2, t % 2
    mate = t + 1 - 2 * core
    cross = (t + n // 2) % n
    leads = core == f % 2
    owner = f == t

    def near(c):
        return c + upper * (n - 1 - 2 * c)

    def far(c):
        return n - 1 - c + upper * (2 * c - n + 1)

    def rows_at(start, size):
        return pl.ds(start if isinstance(start, int) else pl.multiple_of(start, size), size)

    def side(h):
        return rows_at(h * half, half)

    small = [
        pltpu.make_async_copy(source, target, small_sem.at[i])
        for i, (source, target) in enumerate(
            (
                (tok_hbm, tok_ref), (gain_hbm, gain_ref), (post_hbm, post_ref),
                (cos_hbm, cos_ref), (sin_hbm, sin_ref),
            )
        )
    ]
    for fetch in small:
        fetch.start()
    fetches = []
    for g in range(kv):
        for ref, first, size in (
            (wq_hbm, 0, per * HEAD_DIM),
            (wk_hbm, per * HEAD_DIM, HEAD_DIM),
            (wv_hbm, (per + 1) * HEAD_DIM, HEAD_DIM),
        ):
            fetches.append(
                pltpu.make_async_copy(
                    ref.at[:, pl.ds(g * size, size)],
                    w_all.at[g, :, pl.ds(first, size)],
                    w_sem.at[len(fetches)],
                )
            )
    fetches.append(pltpu.make_async_copy(wo_hbm, wo, w_sem.at[len(fetches)]))
    for fetch in fetches:
        fetch.start()

    for fetch in small[:2]:
        fetch.wait()
    tok = tok_ref[...].astype(jnp.float32)
    ss_mine[...] = row_sums(tok * tok)
    finish_greeting()

    def total_out(k, slot):
        return remote(
            ss_mine, ss_got.at[slot], ss_send.at[k - 1], ss_recv.at[slot], f, (t + k) % n
        )

    for k in range(1, n):
        total_out(k, t).start()
    total = ss_mine[...]
    for k in range(1, n):
        slot = (t + k) % n
        total_out(k, slot).wait_recv()
        total = total + ss_got[slot]
    scale = lax.rsqrt(as_column(total) / total_width + eps_norm)
    for i in range(lanes):
        cols = slice(i * 128, (i + 1) * 128)
        xn[:, cols] = (
            tok_ref[:, cols].astype(jnp.float32) * scale * gain_ref[cols].astype(jnp.float32)[None, :]
        ).astype(jnp.bfloat16)

    @pl.when(owner)
    def _():
        xs[f] = xn[...]

    fetches = small[2:] + fetches

    def is_outer(r):
        return (r == 0) | (r == n - 1)

    quarter, eighth = half // 2, half // 4
    away = jnp.logical_not(owner)
    detours = jnp.logical_not(is_outer(f)) & (plane != upper)
    relays = jnp.logical_not(is_outer(f)) & (plane == upper)

    def direct(h):
        return remote(
            xn.at[side(h)], xs.at[f, side(h)], src_send.at[h], x_recv.at[f, h], t, t
        )

    def to_relay(h):
        return remote(
            xn.at[side(h)], relay_buf.at[h], src_send.at[h], relay_recv.at[h], f, cross
        )

    def relayed(h):
        return remote(
            relay_buf.at[h], xs.at[f, side(h)], relay_send.at[h], x_recv.at[f, h], cross, t
        )

    def to_mate(r, h):
        spot = xs.at[r, side(h)]
        return remote(spot, spot, mate_send.at[r, h], x_recv.at[r, h], f, mate)

    def to_cross(r, h):
        spot = xs.at[r, side(h)]
        return remote(spot, spot, cross_send.at[r, h], x_recv.at[r, h], f, cross)

    def send_away(h):
        pl.when(away & jnp.logical_not(detours))(lambda: direct(h).start())
        pl.when(detours)(lambda: to_relay(h).start())

    def relay(h):
        @pl.when(relays)
        def _():
            to_relay(h).wait_recv()
            relayed(h).start()

    def enters(r):
        by_owner = is_outer(r) | (r // 2 == upper)
        return leads & ((by_owner & owner) | jnp.logical_not(by_owner | owner))

    def spread(r, h, roles=(ENTRY, OTHER, LAST)):
        enter = enters(r)
        parts = {ENTRY: enter, OTHER: leads & jnp.logical_not(enter), LAST: jnp.logical_not(leads)}
        active = parts[roles[0]]
        for role in roles[1:]:
            active = active | parts[role]

        @pl.when(active & jnp.logical_not(owner & (r == f)))
        def _():
            to_mate(r, h).wait_recv()

        if ENTRY in roles:
            pl.when(enter)(lambda: to_cross(r, h).start())
        if roles != (LAST,):
            pl.when(active & leads)(lambda: to_mate(r, h).start())

    def place(k):
        j = k // kv
        return j // 2, j % 2, k % kv

    def partial(seq, h, g):
        return jnp.dot(xs[seq, side(h)], w_all[g], preferred_element_type=jnp.float32)

    def near_hop(k, recv):
        landing = near_got if recv is near_recv else far_got
        return remote(
            near_stage.at[k], landing.at[k], near_send.at[k], recv.at[k], inward, t
        )

    def far_hop(k):
        return remote(
            far_stage.at[k], far_got.at[k], far_send.at[k], far_recv.at[k], outward, t
        )

    def first_near(k):
        c, h, g = place(k)
        near_stage[k] = partial(near(c), h, g).astype(jnp.bfloat16)
        near_hop(k, near_recv).start()

    def middle_near(k):
        c, h, g = place(k)
        part = partial(near(c), h, g)
        near_hop(k, near_recv).wait_recv()
        near_stage[k] = (part + near_got[k].astype(jnp.float32)).astype(jnp.bfloat16)
        near_hop(k, far_recv).start()

    def middle_far(k):
        c, h, g = place(k)
        part = partial(far(c), h, g)
        far_hop(k).wait_recv()
        far_stage[k] = (part + far_got[k].astype(jnp.float32)).astype(jnp.bfloat16)
        far_hop(k).start()

    def share(s, h, g, there):
        return remote(
            att.at[s, g, side(h)], att.at[s, g, side(h)],
            att_send.at[s, h, g], att_recv.at[s, h, g], there, t,
        )

    def turn(u, span):
        other = pltpu.roll(u, HEAD_DIM // 2, 1)
        return (u * cos_ref[span] + other * sin_ref[span]).astype(jnp.bfloat16)

    def attend_piece(c, h, g):
        k = (c * 2 + h) * kv + g
        span, seen = slice(h * half, (h + 1) * half), (h + 1) * half
        part = partial(far(c), h, g)
        far_hop(k).wait_recv()
        raw = part + far_got[k].astype(jnp.float32)
        heads = [raw[:, i * HEAD_DIM : (i + 1) * HEAD_DIM] for i in range(per + 2)]
        keys[c, g, span] = turn(heads[per], span)
        values[c, g, span] = heads[per + 1].astype(jnp.bfloat16)
        query = jnp.concatenate([turn(u, span) for u in heads[:per]], axis=0)
        scores = lax.dot_general(
            query, keys[c, g, :seen], (((1,), (1,)), ((), ())),
            preferred_element_type=jnp.float32,
        )
        capped = soft_cap * jnp.tanh(scores * (attn_scale / soft_cap))
        index = lax.broadcasted_iota(jnp.int32, (half, seen), 0) + h * half
        allowed = lax.broadcasted_iota(jnp.int32, (half, seen), 1) <= index
        allowed = jnp.concatenate([allowed] * per, axis=0)
        e = jnp.where(allowed, jnp.exp(capped), 0.0)
        inverse = 1.0 / jnp.sum(e, axis=1, keepdims=True)
        probs = (e * inverse).astype(jnp.bfloat16)
        mixed = jnp.dot(probs, values[c, g, :seen], preferred_element_type=jnp.float32)
        for i in range(per):
            att[far(c), g, span, i * HEAD_DIM : (i + 1) * HEAD_DIM] = mixed[
                i * half : (i + 1) * half
            ].astype(jnp.bfloat16)
        share(far(c), h, g, inward).start()

    def part_hop(s, h):
        m = 2 * s + h
        return remote(
            part_stage.at[m, rows_at((1 - core) * quarter, quarter)], part_got.at[m],
            part_send.at[m], part_recv.at[m], f, mate,
        )

    def pair_hop(s, h):
        m = 2 * s + h
        return remote(
            pair_stage.at[m], pair_got.at[m], pair_send.at[m], pair_recv.at[m], f, cross
        )

    def sum_hop(s, h):
        m = 2 * s + h
        piece = core * 2 + plane
        return remote(
            sum_stage.at[m], proj.at[rows_at(h * half + piece * eighth, eighth)],
            sum_send.at[m], sum_recv.at[h, piece], s, f,
        )

    def pair_sum(m, which):
        kept = part_stage[m, rows_at(core * quarter + which * eighth, eighth)]
        got = part_got[m, rows_at(which * eighth, eighth)]
        return kept.astype(jnp.float32) + got.astype(jnp.float32)

    def out_first(s, h):
        m = 2 * s + h
        acc = jnp.dot(att[s, 0, side(h)], wo[: per * HEAD_DIM], preferred_element_type=jnp.float32)
        for g in range(1, kv):
            acc = acc + jnp.dot(
                att[s, g, side(h)],
                wo[g * per * HEAD_DIM : (g + 1) * per * HEAD_DIM],
                preferred_element_type=jnp.float32,
            )
        part_stage[m] = acc.astype(jnp.bfloat16)
        part_hop(s, h).start()

    def out_second(s, h):
        m = 2 * s + h
        part_hop(s, h).wait_recv()
        pair_stage[m] = pair_sum(m, 1 - plane).astype(jnp.bfloat16)
        pair_hop(s, h).start()

    def out_third(s, h):
        m = 2 * s + h
        pair_hop(s, h).wait_recv()
        summed = pair_sum(m, plane) + pair_got[m].astype(jnp.float32)
        stays = (s == f) & owner

        @pl.when(stays)
        def _():
            start = h * half + (core * 2 + plane) * eighth
            proj[rows_at(start, eighth)] = summed.astype(jnp.bfloat16)

        @pl.when(jnp.logical_not(stays))
        def _():
            sum_stage[m] = summed.astype(jnp.bfloat16)
            sum_hop(s, h).start()

    def advance(i, where):
        out_first(*where(i))
        pl.when(i >= 1)(lambda: out_second(*where(i - 1)))
        pl.when(i >= 2)(lambda: out_third(*where(i - 2)))

    def flush(where):
        out_second(*where(2 * n - 1))
        out_third(*where(2 * n - 2))
        out_third(*where(2 * n - 1))

    @pl.when(at_end)
    def _():
        def where(i):
            j = i % n
            c = j // 2
            return jnp.where(i < n, far(c), near(c)), j % 2

        for h in range(2):
            send_away(h)
        for fetch in fetches[:-1]:
            fetch.wait()
        @pl.when(owner)
        def _():
            for h in range(2):
                spread(f, h)
            for h in range(2):
                to_cross(f, h).wait_send()

        for h in range(2):
            pl.when(away)(lambda h=h: spread(near(0), h))
            loop(h * kv, (h + 1) * kv, first_near)
        for h in range(2):
            spread(far(0), h)
            spread(near(1), h)
            loop((2 + h) * kv, (3 + h) * kv, first_near)
        for h in range(2):
            spread(far(1), h, (ENTRY,))
        fetches[-1].wait()

        def chunk(c):
            for h in range(2):
                pl.when(c == 1)(lambda h=h: spread(far(1), h, (OTHER, LAST)))
                loop(0, kv, lambda g: attend_piece(c, h, g))
                advance(2 * c + h, where)

        loop(0, 2, chunk)

        def gather(i):
            s, h = where(i)
            for g in range(kv):
                share(s, h, g, inward).wait_recv()
            advance(i, where)

        loop(n, 2 * n, gather)
        flush(where)

    @pl.when(in_middle)
    def _():
        def where(i):
            j = i // 2
            c = j // 2
            return jnp.where(i % 2 == 0, far(c), near(c)), j % 2

        for h in range(2):
            send_away(h)
        for fetch in fetches:
            fetch.wait()
        for h in range(2):
            spread(near(0), h)
        relay(0)
        spread(far(0), 0)
        relay(1)
        plan = (
            (far(0), 1, (0, 2, 4)), (near(1), 0, (1, 4, 6)), (near(1), 1, (1, 5, 8)),
            (far(1), 0, (1, 4, 8)), (far(1), 1, (2, 6, 10)),
        )

        def pass_on(k, seq, there):
            c, h, g = place(k)
            share(seq(c), h, g, there).wait_recv()
            share(seq(c), h, g, there).start()

        def step(s):
            for seq, h, steps in plan:
                for role, at in enumerate(steps):
                    pl.when(s == at)(lambda seq=seq, h=h, role=role: spread(seq, h, (role,)))
            pl.when(s < count)(lambda: middle_near(s))
            pl.when((s >= LAG) & (s < count + LAG))(lambda: middle_far(s - LAG))
            for j in range(FAR_PACE):
                k = (s - FAR_AT) * FAR_PACE + j
                pl.when((k >= 0) & (k < count))(lambda k=k: pass_on(k, far, inward))
            for j in range(NEAR_PACE):
                k = (s - NEAR_AT) * NEAR_PACE + j
                pl.when((k >= 0) & (k < count))(lambda k=k: pass_on(k, near, outward))
            m = s - OUT_AT
            pl.when(m >= 0)(lambda: advance(m, where))

        loop(0, OUT_AT + 2 * n, step)
        flush(where)

    def post_out(h, k, slot):
        return remote(
            post_mine.at[h], post_got.at[h, slot],
            post_send.at[h, k - 1], post_recv.at[h, slot], f, (t + k) % n,
        )

    for h in range(2):
        for piece in range(n):
            mine = owner & (core * 2 + plane == piece)

            @pl.when(jnp.logical_not(mine))
            def _():
                spot = proj.at[rows_at(h * half + piece * eighth, eighth)]
                remote(
                    spot, spot, sum_send.at[0], sum_recv.at[h, piece], f, t
                ).wait_recv()

        branch = proj[side(h)].astype(jnp.float32)
        post_mine[h] = row_sums(branch * branch)
        for k in range(1, n):
            post_out(h, k, t).start()
    for h in range(2):
        total = post_mine[h]
        for k in range(1, n):
            slot = (t + k) % n
            post_out(h, k, slot).wait_recv()
            total = total + post_got[h, slot]
        scale = lax.rsqrt(as_column(total) / total_width + eps_norm)
        for i in range(lanes):
            cols = slice(i * 128, (i + 1) * 128)
            out_ref[side(h), cols] = tok_ref[side(h), cols].astype(jnp.float32) + (
                proj[side(h), cols].astype(jnp.float32) * scale * post_ref[cols].astype(jnp.float32)[None, :]
            )

    for k in range(1, n):
        total_out(k, t).wait_send()
        for h in range(2):
            post_out(h, k, t).wait_send()

    for h in range(2):
        pl.when(away)(lambda: direct(h).wait_send())
        pl.when(relays)(lambda: relayed(h).wait_send())

    def drain(r):
        for h in range(2):
            waited = owner & (r == f) & is_outer(r)
            pl.when(enters(r) & jnp.logical_not(waited))(lambda: to_cross(r, h).wait_send())
            pl.when(leads)(lambda: to_mate(r, h).wait_send())

        for h in range(2):
            part_hop(r, h).wait_send()
            pair_hop(r, h).wait_send()
            pl.when(jnp.logical_not((r == f) & owner))(lambda: sum_hop(r, h).wait_send())
            sent = in_middle | (r == far(0)) | (r == far(1))

            @pl.when(sent)
            def _():
                for g in range(kv):
                    share(r, h, g, inward).wait_send()

    loop(0, n, drain)

    def drain_hops(k):
        near_hop(k, far_recv).wait_send()
        pl.when(in_middle)(lambda: far_hop(k).wait_send())

    loop(0, count, drain_hops)


def whole_block(n, tokens, gain, post_gain, cosine, sine, w_query, w_key, w_value, w_out):
    rows, width = tokens.shape
    half, kv = rows // 2, w_key.shape[1] // HEAD_DIM
    per = w_query.shape[1] // w_key.shape[1]
    wide = (per + 2) * HEAD_DIM
    count = 4 * kv
    dma = pltpu.SemaphoreType.DMA
    bf16 = lambda *shape: pltpu.VMEM(shape, jnp.bfloat16)
    f32 = lambda *shape: pltpu.VMEM(shape, jnp.float32)
    vmem = pl.BlockSpec(memory_space=pltpu.VMEM)
    in_hbm = pl.BlockSpec(memory_space=pltpu.HBM)
    return pl.pallas_call(
        functools.partial(block_kernel, n),
        out_shape=pltpu.VMEM((rows, width), jnp.float32),
        in_specs=[in_hbm] * 9,
        out_specs=vmem,
        scratch_shapes=[
            bf16(rows, width), bf16(width), bf16(width), f32(rows, HEAD_DIM), f32(rows, HEAD_DIM),
            dma((5,)),
            bf16(kv, width, wide), bf16(*w_out.shape), bf16(rows, width),
            bf16(n, rows, width), bf16(2, half, width), f32(8, rows), f32(n, 8, rows),
            bf16(count, half, wide), bf16(count, half, wide),
            bf16(count, half, wide), bf16(count, half, wide),
            bf16(2, kv, rows, HEAD_DIM), bf16(2, kv, rows, HEAD_DIM),
            bf16(n, kv, rows, per * HEAD_DIM),
            bf16(2 * n, half, width), bf16(2 * n, half // 2, width),
            bf16(2 * n, half // 4, width), bf16(2 * n, half // 4, width),
            bf16(2 * n, half // 4, width), bf16(rows, width),
            f32(2, 8, half), f32(2, n, 8, half),
            dma((3 * kv + 1,)), dma((n - 1,)), dma((n,)), dma((2,)), dma((2,)), dma((2,)),
            dma((n, 2)), dma((n, 2)), dma((n, 2)),
            dma((count,)), dma((count,)), dma((count,)), dma((count,)),
            dma((n, 2, kv)), dma((n, 2, kv)),
            dma((2 * n,)), dma((2 * n,)), dma((2 * n,)), dma((2 * n,)),
            dma((2 * n,)), dma((2, n)),
            dma((2, n - 1)), dma((2, n)),
        ],
        compiler_params=pltpu.CompilerParams(
            collective_id=0, has_side_effects=True, vmem_limit_bytes=VMEM_LIMIT
        ),
    )(tokens, gain, post_gain, cosine, sine, w_query, w_key, w_value, w_out)


def tables(rows):
    half = HEAD_DIM // 2
    freq = np.float32(rope_base) ** (-(np.arange(half, dtype=np.float32) * np.float32(2.0 / HEAD_DIM)))
    angle = np.arange(rows, dtype=np.float32)[:, None] * freq[None, :].astype(np.float32)
    cosine, sine = np.cos(angle), np.sin(angle)
    return (
        jnp.asarray(np.concatenate([cosine, cosine], axis=1), jnp.float32),
        jnp.asarray(np.concatenate([-sine, sine], axis=1), jnp.float32),
    )


def solution(mesh):
    n_fsdp, n_tensor = mesh.shape["fsdp"], mesh.shape["tensor"]

    def on_device(tokens, norm_gain, w_query, w_key, w_value, w_out, post_gain):
        rows = tokens.shape[0]
        width = tokens.shape[1] * n_tensor
        if n_fsdp == n_tensor == CHAIN:
            return whole_block(
                n_fsdp, tokens, norm_gain, post_gain, *tables(rows), w_query, w_key, w_value, w_out
            )
        widened = tokens.astype(jnp.float32)
        total = lax.psum(jnp.sum(widened * widened, axis=1), "tensor")
        normed = (
            widened * lax.rsqrt(total / width + eps_norm)[:, None] * norm_gain.astype(jnp.float32)
        ).astype(jnp.bfloat16)
        mine = to_rows(normed, n_fsdp, n_tensor)
        raw = []
        for piece in (w_query, w_key, w_value):
            part = jnp.dot(mine, piece, preferred_element_type=jnp.float32).astype(jnp.bfloat16)
            parts = lax.all_to_all(part, "fsdp", 0, 0, tiled=True)
            parts = parts.reshape(n_fsdp, rows, piece.shape[1])
            raw.append(jnp.sum(parts.astype(jnp.float32), axis=0))
        query_raw, key_raw, value_raw = raw
        position = jnp.arange(rows, dtype=jnp.int32)
        local_heads = w_query.shape[1] // HEAD_DIM
        local_kv = w_key.shape[1] // HEAD_DIM
        query = rotate(query_raw.reshape(rows, local_heads, HEAD_DIM), position)
        key = rotate(key_raw.reshape(rows, local_kv, HEAD_DIM), position)
        query, key = query.astype(jnp.bfloat16), key.astype(jnp.bfloat16)
        value = value_raw.astype(jnp.bfloat16).reshape(rows, local_kv, HEAD_DIM)
        attn = attend(query, key, value, position)
        attn_all = lax.all_gather(attn, "fsdp", axis=0, tiled=True)
        part = jnp.dot(attn_all, w_out, preferred_element_type=jnp.float32).astype(jnp.bfloat16)
        summed = lax.psum_scatter(part, "tensor", scatter_dimension=0, tiled=True)
        proj = from_rows(summed, rows, n_fsdp, n_tensor).astype(jnp.float32)
        post_total = lax.psum(jnp.sum(proj * proj, axis=1), "tensor")
        branch = (
            proj
            * lax.rsqrt(post_total / width + eps_norm)[:, None]
            * post_gain.astype(jnp.float32)
        )
        return tokens.astype(jnp.float32) + branch

    placed = (
        P(("groups", "fsdp"), "tensor"),
        P("tensor"),
        P("fsdp", "tensor"),
        P("fsdp", "tensor"),
        P("fsdp", "tensor"),
        P("tensor", "fsdp"),
        P("tensor"),
    )
    return jax.shard_map(
        on_device,
        mesh=mesh,
        in_specs=placed,
        out_specs=P(("groups", "fsdp"), "tensor"),
        check_vma=False,
    )
```

```python
import functools

import jax
import numpy as np
import jax.numpy as jnp
from jax import lax
from jax.experimental import pallas as pl
from jax.experimental.pallas import tpu as pltpu
from jax.sharding import PartitionSpec as P

HEAD_DIM = 128

eps_norm = 1e-06
soft_cap = 50.0
attn_scale = 144.0 ** (-0.5)
rope_base = 10000.0


def rotate(values, position):
    head_dim = values.shape[-1]
    half = head_dim // 2
    freq = rope_base ** (-(jnp.arange(half, dtype=jnp.float32) * 2.0 / head_dim))
    angle = position.astype(jnp.float32)[:, None] * freq[None, :]
    cosine = jnp.cos(angle)[:, None, :]
    sine = jnp.sin(angle)[:, None, :]
    first = values[..., :half]
    second = values[..., half:]
    return jnp.concatenate(
        [first * cosine - second * sine, second * cosine + first * sine], axis=-1
    )


def attend(query, keys, values, position):
    count, heads, head_dim = query.shape
    kv_count = keys.shape[1]
    grouped = query.reshape(count, kv_count, heads // kv_count, head_dim)
    scores = (
        jnp.einsum("nkgd,mkd->kgnm", grouped, keys, preferred_element_type=jnp.float32) * attn_scale
    )
    capped = soft_cap * jnp.tanh(scores / soft_cap)
    allowed = position[None, :] <= position[:, None]
    weights = jnp.where(allowed, jnp.exp(capped), 0.0)
    probs = (weights / jnp.sum(weights, axis=-1, keepdims=True)).astype(jnp.bfloat16)
    mixed = jnp.einsum("kgnm,mkd->nkgd", probs, values, preferred_element_type=jnp.float32)
    return mixed.reshape(count, heads * head_dim).astype(jnp.bfloat16)


def swap_pairs(n_fsdp, n_tensor, turn):
    ratio = n_fsdp // n_tensor
    pairs = []
    for f in range(n_fsdp):
        for t in range(n_tensor):
            j = (f + turn) % ratio
            pairs.append((f * n_tensor + t, (t * ratio + j) * n_tensor + f // ratio))
    return pairs


def to_rows(block, n_fsdp, n_tensor):
    rows = block.shape[0]
    ratio = n_fsdp // n_tensor
    width = block.shape[1] // ratio
    f = lax.axis_index("fsdp")
    if ratio == 1:
        held = lax.ppermute(block, ("fsdp", "tensor"), swap_pairs(n_fsdp, n_tensor, 0))
    else:
        held = jnp.zeros((ratio, rows, width), block.dtype)
        for turn in range(ratio):
            piece = lax.dynamic_slice_in_dim(block, (f + turn) % ratio * width, width, 1)
            got = lax.ppermute(piece, ("fsdp", "tensor"), swap_pairs(n_fsdp, n_tensor, turn))
            held = lax.dynamic_update_index_in_dim(held, got, (f - turn) % ratio, 0)
        held = held.reshape(ratio * rows, width)
    return lax.all_gather(held, "tensor", axis=0, tiled=True)


def from_rows(summed, rows, n_fsdp, n_tensor):
    ratio = n_fsdp // n_tensor
    width = summed.shape[1]
    f = lax.axis_index("fsdp")
    back = lambda turn: [(b, a) for a, b in swap_pairs(n_fsdp, n_tensor, turn)]
    if ratio == 1:
        return lax.ppermute(summed, ("fsdp", "tensor"), back(0))
    pieces = summed.reshape(ratio, rows, width)
    out = jnp.zeros((rows, ratio * width), summed.dtype)
    for turn in range(ratio):
        piece = lax.dynamic_index_in_dim(pieces, (f - turn) % ratio, 0, keepdims=False)
        got = lax.ppermute(piece, ("fsdp", "tensor"), back(turn))
        out = lax.dynamic_update_slice_in_dim(out, got, (f + turn) % ratio * width, 1)
    return out


MESH = pl.DeviceIdType.MESH
VMEM_LIMIT = 60 * 1024 * 1024
CHAIN = 4
LAG = 3
FAR_AT, FAR_RUSH = 15, 18
NEAR_AT, NEAR_PACE = 17, 2
OUT_AT = 17
EARLY = 2
HOLD = 3
ENTRY, OTHER, LAST = 0, 1, 2


def remote(src, dst, send, recv, a, b):
    return pltpu.make_async_remote_copy(
        src_ref=src,
        dst_ref=dst,
        send_sem=send,
        recv_sem=recv,
        device_id={"fsdp": a, "tensor": b},
        device_id_type=MESH,
    )


def greet(n, f, t):
    barrier = pltpu.get_barrier_semaphore()
    for a in range(n):
        for b in range(n):
            @pl.when(jnp.logical_not((f == a) & (t == b)))
            def _():
                pl.semaphore_signal(
                    barrier, inc=1, device_id={"fsdp": a, "tensor": b}, device_id_type=MESH
                )
    return lambda: pl.semaphore_wait(barrier, n * n - 1)


def loop(low, high, body):
    def step(i, carry):
        body(i)
        return carry

    lax.fori_loop(low, high, step, 0)


def row_sums(squares):
    groups = squares.shape[1] // 128
    lanes = squares[:, :128]
    for i in range(1, groups):
        lanes = lanes + squares[:, i * 128 : (i + 1) * 128]
    row = jnp.sum(lanes.T, axis=0, keepdims=True)
    return jnp.broadcast_to(row, (8, squares.shape[0]))


def as_column(row):
    return jnp.broadcast_to(row[:1], (128, row.shape[1])).T


def block_kernel(
    n, tok_hbm, gain_hbm, post_hbm, cos_hbm, sin_hbm, wq_hbm, wk_hbm, wv_hbm, wo_hbm, out_ref,
    tok_ref, gain_ref, post_ref, cos_ref, sin_ref, small_sem, w_all, wo, xn, xs, relay_buf, ss_mine, ss_got,
    near_stage, far_stage, near_got, far_got, keys, values, att,
    part_stage, part_got, pair_stage, pair_got, sum_stage, proj, post_mine, post_got,
    w_sem, ss_send, ss_recv, src_send, relay_recv, relay_send,
    x_recv, mate_send, cross_send, near_send, near_recv, far_send, far_recv,
    att_send, att_recv, part_send, part_recv, pair_send, pair_recv, sum_send, sum_recv,
    post_send, post_recv,
):
    f, t = lax.axis_index("fsdp"), lax.axis_index("tensor")
    rows, width = tok_ref.shape
    half = rows // 2
    kv = w_all.shape[0]
    per = att.shape[3] // HEAD_DIM
    count = 4 * kv
    lanes = width // 128
    total_width = width * n
    finish_greeting = greet(n, f, t)

    upper = f // 2
    inward = f + 1 - 2 * upper
    outward = f - 1 + 2 * upper
    at_end = (f == 0) | (f == n - 1)
    in_middle = (f > 0) & (f < n - 1)
    plane, core = t // 2, t % 2
    mate = t + 1 - 2 * core
    cross = (t + n // 2) % n
    leads = core == f % 2
    owner = f == t

    def near(c):
        return c + upper * (n - 1 - 2 * c)

    def far(c):
        return n - 1 - c + upper * (2 * c - n + 1)

    def rows_at(start, size):
        return pl.ds(start if isinstance(start, int) else pl.multiple_of(start, size), size)

    def side(h):
        return rows_at(h * half, half)

    small = [
        pltpu.make_async_copy(source, target, small_sem.at[i])
        for i, (source, target) in enumerate(
            (
                (tok_hbm, tok_ref), (gain_hbm, gain_ref), (post_hbm, post_ref),
                (cos_hbm, cos_ref), (sin_hbm, sin_ref),
            )
        )
    ]
    for fetch in small:
        fetch.start()
    fetches = []
    for g in range(kv):
        for ref, first, size in (
            (wq_hbm, 0, per * HEAD_DIM),
            (wk_hbm, per * HEAD_DIM, HEAD_DIM),
            (wv_hbm, (per + 1) * HEAD_DIM, HEAD_DIM),
        ):
            fetches.append(
                pltpu.make_async_copy(
                    ref.at[:, pl.ds(g * size, size)],
                    w_all.at[g, :, pl.ds(first, size)],
                    w_sem.at[len(fetches)],
                )
            )
    fetches.append(pltpu.make_async_copy(wo_hbm, wo, w_sem.at[len(fetches)]))
    for fetch in fetches:
        fetch.start()

    for fetch in small[:2]:
        fetch.wait()
    tok = tok_ref[...].astype(jnp.float32)
    ss_mine[...] = row_sums(tok * tok)
    finish_greeting()

    def total_out(k, slot):
        return remote(
            ss_mine, ss_got.at[slot], ss_send.at[k - 1], ss_recv.at[slot], f, (t + k) % n
        )

    for k in range(1, n):
        total_out(k, t).start()
    total = ss_mine[...]
    for k in range(1, n):
        slot = (t + k) % n
        total_out(k, slot).wait_recv()
        total = total + ss_got[slot]
    scale = lax.rsqrt(as_column(total) / total_width + eps_norm)
    for i in range(lanes):
        cols = slice(i * 128, (i + 1) * 128)
        xn[:, cols] = (
            tok_ref[:, cols].astype(jnp.float32) * scale * gain_ref[cols].astype(jnp.float32)[None, :]
        ).astype(jnp.bfloat16)

    @pl.when(owner)
    def _():
        xs[f] = xn[...]

    fetches = small[2:] + fetches

    def is_outer(r):
        return (r == 0) | (r == n - 1)

    quarter, eighth = half // 2, half // 4
    away = jnp.logical_not(owner)
    detours = jnp.logical_not(is_outer(f)) & (plane != upper)
    relays = jnp.logical_not(is_outer(f)) & (plane == upper)

    def direct(h):
        return remote(
            xn.at[side(h)], xs.at[f, side(h)], src_send.at[h], x_recv.at[f, h], t, t
        )

    def to_relay(h):
        return remote(
            xn.at[side(h)], relay_buf.at[h], src_send.at[h], relay_recv.at[h], f, cross
        )

    def relayed(h):
        return remote(
            relay_buf.at[h], xs.at[f, side(h)], relay_send.at[h], x_recv.at[f, h], cross, t
        )

    def to_mate(r, h):
        spot = xs.at[r, side(h)]
        return remote(spot, spot, mate_send.at[r, h], x_recv.at[r, h], f, mate)

    def to_cross(r, h):
        spot = xs.at[r, side(h)]
        return remote(spot, spot, cross_send.at[r, h], x_recv.at[r, h], f, cross)

    def send_away(h):
        pl.when(away & jnp.logical_not(detours))(lambda: direct(h).start())
        pl.when(detours)(lambda: to_relay(h).start())

    def relay(h):
        @pl.when(relays)
        def _():
            to_relay(h).wait_recv()
            relayed(h).start()

    def enters(r):
        by_owner = is_outer(r) | (r // 2 == upper)
        return leads & ((by_owner & owner) | jnp.logical_not(by_owner | owner))

    def spread(r, h, roles=(ENTRY, OTHER, LAST)):
        enter = enters(r)
        parts = {ENTRY: enter, OTHER: leads & jnp.logical_not(enter), LAST: jnp.logical_not(leads)}
        active = parts[roles[0]]
        for role in roles[1:]:
            active = active | parts[role]

        @pl.when(active & jnp.logical_not(owner & (r == f)))
        def _():
            to_mate(r, h).wait_recv()

        if ENTRY in roles:
            pl.when(enter)(lambda: to_cross(r, h).start())
        if roles != (LAST,):
            pl.when(active & leads)(lambda: to_mate(r, h).start())

    def place(k):
        j = k // kv
        return j // 2, j % 2, k % kv

    def partial(seq, h, g):
        return jnp.dot(xs[seq, side(h)], w_all[g], preferred_element_type=jnp.float32)

    def near_hop(k, recv):
        landing = near_got if recv is near_recv else far_got
        return remote(
            near_stage.at[k], landing.at[k], near_send.at[k], recv.at[k], inward, t
        )

    def far_hop(k):
        return remote(
            far_stage.at[k], far_got.at[k], far_send.at[k], far_recv.at[k], outward, t
        )

    def first_near(k):
        c, h, g = place(k)
        near_stage[k] = partial(near(c), h, g).astype(jnp.bfloat16)
        near_hop(k, near_recv).start()

    def middle_near(k):
        c, h, g = place(k)
        part = partial(near(c), h, g)
        near_hop(k, near_recv).wait_recv()
        near_stage[k] = (part + near_got[k].astype(jnp.float32)).astype(jnp.bfloat16)
        near_hop(k, far_recv).start()

    def middle_far(k):
        c, h, g = place(k)
        part = partial(far(c), h, g)
        far_hop(k).wait_recv()
        far_stage[k] = (part + far_got[k].astype(jnp.float32)).astype(jnp.bfloat16)
        far_hop(k).start()

    def share(s, h, g, there):
        return remote(
            att.at[s, g, side(h)], att.at[s, g, side(h)],
            att_send.at[s, h, g], att_recv.at[s, h, g], there, t,
        )

    def turn(u, span):
        other = pltpu.roll(u, HEAD_DIM // 2, 1)
        return (u * cos_ref[span] + other * sin_ref[span]).astype(jnp.bfloat16)

    def attend_piece(c, h, g):
        k = (c * 2 + h) * kv + g
        span, seen = slice(h * half, (h + 1) * half), (h + 1) * half
        part = partial(far(c), h, g)
        far_hop(k).wait_recv()
        raw = part + far_got[k].astype(jnp.float32)
        heads = [raw[:, i * HEAD_DIM : (i + 1) * HEAD_DIM] for i in range(per + 2)]
        keys[c, g, span] = turn(heads[per], span)
        values[c, g, span] = heads[per + 1].astype(jnp.bfloat16)
        query = jnp.concatenate([turn(u, span) for u in heads[:per]], axis=0)
        scores = lax.dot_general(
            query, keys[c, g, :seen], (((1,), (1,)), ((), ())),
            preferred_element_type=jnp.float32,
        )
        capped = soft_cap * jnp.tanh(scores * (attn_scale / soft_cap))
        index = lax.broadcasted_iota(jnp.int32, (half, seen), 0) + h * half
        allowed = lax.broadcasted_iota(jnp.int32, (half, seen), 1) <= index
        allowed = jnp.concatenate([allowed] * per, axis=0)
        e = jnp.where(allowed, jnp.exp(capped), 0.0)
        inverse = 1.0 / jnp.sum(e, axis=1, keepdims=True)
        probs = (e * inverse).astype(jnp.bfloat16)
        mixed = jnp.dot(probs, values[c, g, :seen], preferred_element_type=jnp.float32)
        for i in range(per):
            att[far(c), g, span, i * HEAD_DIM : (i + 1) * HEAD_DIM] = mixed[
                i * half : (i + 1) * half
            ].astype(jnp.bfloat16)
        share(far(c), h, g, inward).start()

    def part_hop(s, h):
        m = 2 * s + h
        return remote(
            part_stage.at[m, rows_at((1 - core) * quarter, quarter)], part_got.at[m],
            part_send.at[m], part_recv.at[m], f, mate,
        )

    def pair_hop(s, h):
        m = 2 * s + h
        return remote(
            pair_stage.at[m], pair_got.at[m], pair_send.at[m], pair_recv.at[m], f, cross
        )

    def sum_hop(s, h):
        m = 2 * s + h
        piece = core * 2 + plane
        return remote(
            sum_stage.at[m], proj.at[rows_at(h * half + piece * eighth, eighth)],
            sum_send.at[m], sum_recv.at[h, piece], s, f,
        )

    def pair_sum(m, which):
        kept = part_stage[m, rows_at(core * quarter + which * eighth, eighth)]
        got = part_got[m, rows_at(which * eighth, eighth)]
        return kept.astype(jnp.float32) + got.astype(jnp.float32)

    def out_first(s, h):
        m = 2 * s + h
        acc = jnp.dot(att[s, 0, side(h)], wo[: per * HEAD_DIM], preferred_element_type=jnp.float32)
        for g in range(1, kv):
            acc = acc + jnp.dot(
                att[s, g, side(h)],
                wo[g * per * HEAD_DIM : (g + 1) * per * HEAD_DIM],
                preferred_element_type=jnp.float32,
            )
        part_stage[m] = acc.astype(jnp.bfloat16)
        part_hop(s, h).start()

    def out_second(s, h):
        m = 2 * s + h
        part_hop(s, h).wait_recv()
        pair_stage[m] = pair_sum(m, 1 - plane).astype(jnp.bfloat16)
        pair_hop(s, h).start()

    def out_third(s, h):
        m = 2 * s + h
        pair_hop(s, h).wait_recv()
        summed = pair_sum(m, plane) + pair_got[m].astype(jnp.float32)
        stays = (s == f) & owner

        @pl.when(stays)
        def _():
            start = h * half + (core * 2 + plane) * eighth
            proj[rows_at(start, eighth)] = summed.astype(jnp.bfloat16)

        @pl.when(jnp.logical_not(stays))
        def _():
            sum_stage[m] = summed.astype(jnp.bfloat16)
            sum_hop(s, h).start()

    @pl.when(at_end)
    def _():
        def where(i):
            j = i % n
            c = j // 2
            return jnp.where(i < n, far(c), near(c)), j % 2

        @pl.when(owner)
        def _():
            for h in range(2):
                spread(f, h)

        send_away(0)
        for fetch in fetches[:-1]:
            fetch.wait()
        pl.when(owner)(lambda: to_cross(f, 0).wait_send())
        pl.when(away)(lambda: spread(near(0), 0))
        loop(0, EARLY, first_near)
        send_away(1)
        loop(EARLY, kv, first_near)
        pl.when(away)(lambda: spread(near(0), 1))
        loop(kv, 2 * kv, first_near)
        for h in range(2):
            spread(near(1), h)
            spread(far(0), h)
            loop((2 + h) * kv, (3 + h) * kv, first_near)
        for h in range(2):
            spread(far(1), h, (ENTRY,))
        fetches[-1].wait()

        def chunk(c):
            for h in range(2):
                pl.when(c == 1)(lambda h=h: spread(far(1), h, (OTHER, LAST)))
                loop(0, kv, lambda g: attend_piece(c, h, g))
                i = 2 * c + h
                out_first(*where(i))
                pl.when(i >= 1)(lambda: out_second(*where(i - 1)))

        loop(0, 2, chunk)

        out_second(*where(n - 1))

        def gather(i):
            s, h = where(i)
            for g in range(kv):
                share(s, h, g, inward).wait_recv()
            out_first(s, h)
            pl.when(i == n + HOLD)(lambda: loop(0, n, lambda j: out_third(*where(j))))
            out_second(s, h)
            out_third(s, h)

        loop(n, 2 * n, gather)

    @pl.when(in_middle)
    def _():
        def where(i):
            j = i // 2
            c = j // 2
            return jnp.where(i % 2 == 0, far(c), near(c)), j % 2

        for h in range(2):
            send_away(h)
        for fetch in fetches:
            fetch.wait()
        spread(near(0), 0)
        plan = (
            (far(0), 0, (0, 1, 2)), (near(0), 1, (2, 3, 4)), (far(0), 1, (2, 4, 5)),
            (near(1), 0, (1, 3, 5)), (far(1), 0, (2, 5, 8)),
            (near(1), 1, (3, 6, 8)), (far(1), 1, (3, 6, 10)),
        )

        def pass_on(k, seq, there):
            c, h, g = place(k)
            share(seq(c), h, g, there).wait_recv()
            share(seq(c), h, g, there).start()

        def step(s):
            for h in range(2):
                pl.when(s == h)(lambda h=h: relay(h))
            for seq, h, steps in plan:
                for role, at in enumerate(steps):
                    pl.when(s == at)(lambda seq=seq, h=h, role=role: spread(seq, h, (role,)))
            pl.when((s >= LAG) & (s < count + LAG))(lambda: middle_far(s - LAG))
            pl.when(s < count)(lambda: middle_near(s))
            late = jnp.maximum(s - FAR_RUSH, 0)
            for j in range(3):
                k = (s - FAR_AT) * 2 + late + j
                due = (s >= FAR_AT) & (k < count)
                if j == 2:
                    due = due & (s >= FAR_RUSH)
                pl.when(due)(lambda k=k: pass_on(k, far, inward))
            m = s - OUT_AT
            pl.when(m >= 1)(lambda: out_second(*where(m - 1)))
            for j in range(NEAR_PACE):
                k = (s - NEAR_AT) * NEAR_PACE + j
                pl.when((k >= 0) & (k < count))(lambda k=k: pass_on(k, near, outward))
            pl.when(m >= 0)(lambda: out_first(*where(m)))

        loop(0, OUT_AT + 2 * n, step)
        loop(0, 2 * n - 1, lambda i: out_third(*where(i)))
        out_second(*where(2 * n - 1))
        out_third(*where(2 * n - 1))

    def post_out(h, k, slot):
        return remote(
            post_mine.at[h], post_got.at[h, slot],
            post_send.at[h, k - 1], post_recv.at[h, slot], f, (t + k) % n,
        )

    for h in range(2):
        for piece in range(n):
            mine = owner & (core * 2 + plane == piece)

            @pl.when(jnp.logical_not(mine))
            def _():
                spot = proj.at[rows_at(h * half + piece * eighth, eighth)]
                remote(
                    spot, spot, sum_send.at[0], sum_recv.at[h, piece], f, t
                ).wait_recv()

        branch = proj[side(h)].astype(jnp.float32)
        post_mine[h] = row_sums(branch * branch)
        for k in range(1, n):
            post_out(h, k, t).start()
    for h in range(2):
        total = post_mine[h]
        for k in range(1, n):
            slot = (t + k) % n
            post_out(h, k, slot).wait_recv()
            total = total + post_got[h, slot]
        scale = lax.rsqrt(as_column(total) / total_width + eps_norm)
        for i in range(lanes):
            cols = slice(i * 128, (i + 1) * 128)
            out_ref[side(h), cols] = tok_ref[side(h), cols].astype(jnp.float32) + (
                proj[side(h), cols].astype(jnp.float32) * scale * post_ref[cols].astype(jnp.float32)[None, :]
            )

    for k in range(1, n):
        total_out(k, t).wait_send()
        for h in range(2):
            post_out(h, k, t).wait_send()

    for h in range(2):
        pl.when(away)(lambda: direct(h).wait_send())
        pl.when(relays)(lambda: relayed(h).wait_send())

    def drain(r):
        for h in range(2):
            waited = owner & (r == f) & is_outer(r) & (h == 0)
            pl.when(enters(r) & jnp.logical_not(waited))(lambda: to_cross(r, h).wait_send())
            pl.when(leads)(lambda: to_mate(r, h).wait_send())

        for h in range(2):
            part_hop(r, h).wait_send()
            pair_hop(r, h).wait_send()
            pl.when(jnp.logical_not((r == f) & owner))(lambda: sum_hop(r, h).wait_send())
            sent = in_middle | (r == far(0)) | (r == far(1))

            @pl.when(sent)
            def _():
                for g in range(kv):
                    share(r, h, g, inward).wait_send()

    loop(0, n, drain)

    def drain_hops(k):
        near_hop(k, far_recv).wait_send()
        pl.when(in_middle)(lambda: far_hop(k).wait_send())

    loop(0, count, drain_hops)


def whole_block(n, tokens, gain, post_gain, cosine, sine, w_query, w_key, w_value, w_out):
    rows, width = tokens.shape
    half, kv = rows // 2, w_key.shape[1] // HEAD_DIM
    per = w_query.shape[1] // w_key.shape[1]
    wide = (per + 2) * HEAD_DIM
    count = 4 * kv
    dma = pltpu.SemaphoreType.DMA
    bf16 = lambda *shape: pltpu.VMEM(shape, jnp.bfloat16)
    f32 = lambda *shape: pltpu.VMEM(shape, jnp.float32)
    vmem = pl.BlockSpec(memory_space=pltpu.VMEM)
    in_hbm = pl.BlockSpec(memory_space=pltpu.HBM)
    return pl.pallas_call(
        functools.partial(block_kernel, n),
        out_shape=pltpu.VMEM((rows, width), jnp.float32),
        in_specs=[in_hbm] * 9,
        out_specs=vmem,
        scratch_shapes=[
            bf16(rows, width), bf16(width), bf16(width), f32(rows, HEAD_DIM), f32(rows, HEAD_DIM),
            dma((5,)),
            bf16(kv, width, wide), bf16(*w_out.shape), bf16(rows, width),
            bf16(n, rows, width), bf16(2, half, width), f32(8, rows), f32(n, 8, rows),
            bf16(count, half, wide), bf16(count, half, wide),
            bf16(count, half, wide), bf16(count, half, wide),
            bf16(2, kv, rows, HEAD_DIM), bf16(2, kv, rows, HEAD_DIM),
            bf16(n, kv, rows, per * HEAD_DIM),
            bf16(2 * n, half, width), bf16(2 * n, half // 2, width),
            bf16(2 * n, half // 4, width), bf16(2 * n, half // 4, width),
            bf16(2 * n, half // 4, width), bf16(rows, width),
            f32(2, 8, half), f32(2, n, 8, half),
            dma((3 * kv + 1,)), dma((n - 1,)), dma((n,)), dma((2,)), dma((2,)), dma((2,)),
            dma((n, 2)), dma((n, 2)), dma((n, 2)),
            dma((count,)), dma((count,)), dma((count,)), dma((count,)),
            dma((n, 2, kv)), dma((n, 2, kv)),
            dma((2 * n,)), dma((2 * n,)), dma((2 * n,)), dma((2 * n,)),
            dma((2 * n,)), dma((2, n)),
            dma((2, n - 1)), dma((2, n)),
        ],
        compiler_params=pltpu.CompilerParams(
            collective_id=0, has_side_effects=True, vmem_limit_bytes=VMEM_LIMIT
        ),
    )(tokens, gain, post_gain, cosine, sine, w_query, w_key, w_value, w_out)


def tables(rows):
    half = HEAD_DIM // 2
    freq = np.float32(rope_base) ** (-(np.arange(half, dtype=np.float32) * np.float32(2.0 / HEAD_DIM)))
    angle = np.arange(rows, dtype=np.float32)[:, None] * freq[None, :].astype(np.float32)
    cosine, sine = np.cos(angle), np.sin(angle)
    return (
        jnp.asarray(np.concatenate([cosine, cosine], axis=1), jnp.float32),
        jnp.asarray(np.concatenate([-sine, sine], axis=1), jnp.float32),
    )


def solution(mesh):
    n_fsdp, n_tensor = mesh.shape["fsdp"], mesh.shape["tensor"]

    def on_device(tokens, norm_gain, w_query, w_key, w_value, w_out, post_gain):
        rows = tokens.shape[0]
        width = tokens.shape[1] * n_tensor
        if n_fsdp == n_tensor == CHAIN:
            return whole_block(
                n_fsdp, tokens, norm_gain, post_gain, *tables(rows), w_query, w_key, w_value, w_out
            )
        widened = tokens.astype(jnp.float32)
        total = lax.psum(jnp.sum(widened * widened, axis=1), "tensor")
        normed = (
            widened * lax.rsqrt(total / width + eps_norm)[:, None] * norm_gain.astype(jnp.float32)
        ).astype(jnp.bfloat16)
        mine = to_rows(normed, n_fsdp, n_tensor)
        raw = []
        for piece in (w_query, w_key, w_value):
            part = jnp.dot(mine, piece, preferred_element_type=jnp.float32).astype(jnp.bfloat16)
            parts = lax.all_to_all(part, "fsdp", 0, 0, tiled=True)
            parts = parts.reshape(n_fsdp, rows, piece.shape[1])
            raw.append(jnp.sum(parts.astype(jnp.float32), axis=0))
        query_raw, key_raw, value_raw = raw
        position = jnp.arange(rows, dtype=jnp.int32)
        local_heads = w_query.shape[1] // HEAD_DIM
        local_kv = w_key.shape[1] // HEAD_DIM
        query = rotate(query_raw.reshape(rows, local_heads, HEAD_DIM), position)
        key = rotate(key_raw.reshape(rows, local_kv, HEAD_DIM), position)
        query, key = query.astype(jnp.bfloat16), key.astype(jnp.bfloat16)
        value = value_raw.astype(jnp.bfloat16).reshape(rows, local_kv, HEAD_DIM)
        attn = attend(query, key, value, position)
        attn_all = lax.all_gather(attn, "fsdp", axis=0, tiled=True)
        part = jnp.dot(attn_all, w_out, preferred_element_type=jnp.float32).astype(jnp.bfloat16)
        summed = lax.psum_scatter(part, "tensor", scatter_dimension=0, tiled=True)
        proj = from_rows(summed, rows, n_fsdp, n_tensor).astype(jnp.float32)
        post_total = lax.psum(jnp.sum(proj * proj, axis=1), "tensor")
        branch = (
            proj
            * lax.rsqrt(post_total / width + eps_norm)[:, None]
            * post_gain.astype(jnp.float32)
        )
        return tokens.astype(jnp.float32) + branch

    placed = (
        P(("groups", "fsdp"), "tensor"),
        P("tensor"),
        P("fsdp", "tensor"),
        P("fsdp", "tensor"),
        P("fsdp", "tensor"),
        P("tensor", "fsdp"),
        P("tensor"),
    )
    return jax.shard_map(
        on_device,
        mesh=mesh,
        in_specs=placed,
        out_specs=P(("groups", "fsdp"), "tensor"),
        check_vma=False,
    )
```

```python
import functools

import jax
import numpy as np
import jax.numpy as jnp
from jax import lax
from jax.experimental import pallas as pl
from jax.experimental.pallas import tpu as pltpu
from jax.sharding import PartitionSpec as P

HEAD_DIM = 128

eps_norm = 1e-06
soft_cap = 50.0
attn_scale = 144.0 ** (-0.5)
rope_base = 10000.0


def rotate(values, position):
    head_dim = values.shape[-1]
    half = head_dim // 2
    freq = rope_base ** (-(jnp.arange(half, dtype=jnp.float32) * 2.0 / head_dim))
    angle = position.astype(jnp.float32)[:, None] * freq[None, :]
    cosine = jnp.cos(angle)[:, None, :]
    sine = jnp.sin(angle)[:, None, :]
    first = values[..., :half]
    second = values[..., half:]
    return jnp.concatenate(
        [first * cosine - second * sine, second * cosine + first * sine], axis=-1
    )


def attend(query, keys, values, position):
    count, heads, head_dim = query.shape
    kv_count = keys.shape[1]
    grouped = query.reshape(count, kv_count, heads // kv_count, head_dim)
    scores = (
        jnp.einsum("nkgd,mkd->kgnm", grouped, keys, preferred_element_type=jnp.float32) * attn_scale
    )
    capped = soft_cap * jnp.tanh(scores / soft_cap)
    allowed = position[None, :] <= position[:, None]
    weights = jnp.where(allowed, jnp.exp(capped), 0.0)
    probs = (weights / jnp.sum(weights, axis=-1, keepdims=True)).astype(jnp.bfloat16)
    mixed = jnp.einsum("kgnm,mkd->nkgd", probs, values, preferred_element_type=jnp.float32)
    return mixed.reshape(count, heads * head_dim).astype(jnp.bfloat16)


def swap_pairs(n_fsdp, n_tensor, turn):
    ratio = n_fsdp // n_tensor
    pairs = []
    for f in range(n_fsdp):
        for t in range(n_tensor):
            j = (f + turn) % ratio
            pairs.append((f * n_tensor + t, (t * ratio + j) * n_tensor + f // ratio))
    return pairs


def to_rows(block, n_fsdp, n_tensor):
    rows = block.shape[0]
    ratio = n_fsdp // n_tensor
    width = block.shape[1] // ratio
    f = lax.axis_index("fsdp")
    if ratio == 1:
        held = lax.ppermute(block, ("fsdp", "tensor"), swap_pairs(n_fsdp, n_tensor, 0))
    else:
        held = jnp.zeros((ratio, rows, width), block.dtype)
        for turn in range(ratio):
            piece = lax.dynamic_slice_in_dim(block, (f + turn) % ratio * width, width, 1)
            got = lax.ppermute(piece, ("fsdp", "tensor"), swap_pairs(n_fsdp, n_tensor, turn))
            held = lax.dynamic_update_index_in_dim(held, got, (f - turn) % ratio, 0)
        held = held.reshape(ratio * rows, width)
    return lax.all_gather(held, "tensor", axis=0, tiled=True)


def from_rows(summed, rows, n_fsdp, n_tensor):
    ratio = n_fsdp // n_tensor
    width = summed.shape[1]
    f = lax.axis_index("fsdp")
    back = lambda turn: [(b, a) for a, b in swap_pairs(n_fsdp, n_tensor, turn)]
    if ratio == 1:
        return lax.ppermute(summed, ("fsdp", "tensor"), back(0))
    pieces = summed.reshape(ratio, rows, width)
    out = jnp.zeros((rows, ratio * width), summed.dtype)
    for turn in range(ratio):
        piece = lax.dynamic_index_in_dim(pieces, (f - turn) % ratio, 0, keepdims=False)
        got = lax.ppermute(piece, ("fsdp", "tensor"), back(turn))
        out = lax.dynamic_update_slice_in_dim(out, got, (f + turn) % ratio * width, 1)
    return out


MESH = pl.DeviceIdType.MESH
VMEM_LIMIT = 60 * 1024 * 1024
CHAIN = 4
LAG = 3
FAR_AT, FAR_RUSH = 15, 18
NEAR_AT, NEAR_PACE = 17, 2
OUT_AT = 17
EARLY = 2
HOLD = 3
ENTRY, OTHER, LAST = 0, 1, 2


def remote(src, dst, send, recv, a, b):
    return pltpu.make_async_remote_copy(
        src_ref=src,
        dst_ref=dst,
        send_sem=send,
        recv_sem=recv,
        device_id={"fsdp": a, "tensor": b},
        device_id_type=MESH,
    )


def greet(n, f, t):
    barrier = pltpu.get_barrier_semaphore()
    for a in range(n):
        for b in range(n):
            @pl.when(jnp.logical_not((f == a) & (t == b)))
            def _():
                pl.semaphore_signal(
                    barrier, inc=1, device_id={"fsdp": a, "tensor": b}, device_id_type=MESH
                )
    return lambda: pl.semaphore_wait(barrier, n * n - 1)


def loop(low, high, body):
    def step(i, carry):
        body(i)
        return carry

    lax.fori_loop(low, high, step, 0)


def row_sums(squares):
    groups = squares.shape[1] // 128
    lanes = squares[:, :128]
    for i in range(1, groups):
        lanes = lanes + squares[:, i * 128 : (i + 1) * 128]
    row = jnp.sum(lanes.T, axis=0, keepdims=True)
    return jnp.broadcast_to(row, (8, squares.shape[0]))


def as_column(row):
    return jnp.broadcast_to(row[:1], (128, row.shape[1])).T


def block_kernel(
    n, tok_hbm, gain_hbm, post_hbm, cos_hbm, sin_hbm, wq_hbm, wk_hbm, wv_hbm, wo_hbm, out_ref,
    tok_ref, gain_ref, post_ref, cos_ref, sin_ref, small_sem, w_all, wo, xn, xs, relay_buf, ss_got, scales, gain_row,
    near_stage, far_stage, near_got, far_got, keys, values, att,
    part_stage, part_got, pair_stage, pair_got, sum_stage, proj, post_mine, post_got,
    w_sem, held_sem, gain_send, gain_recv, ss_send, ss_recv, src_send, relay_recv, relay_send,
    x_recv, mate_send, cross_send, near_send, near_recv, far_send, far_recv,
    att_send, att_recv, part_send, part_recv, pair_send, pair_recv, sum_send, sum_recv,
    post_send, post_recv,
):
    f, t = lax.axis_index("fsdp"), lax.axis_index("tensor")
    rows, width = tok_ref.shape
    half = rows // 2
    kv = w_all.shape[0]
    per = att.shape[3] // HEAD_DIM
    count = 4 * kv
    lanes = width // 128
    total_width = width * n
    finish_greeting = greet(n, f, t)

    upper = f // 2
    inward = f + 1 - 2 * upper
    outward = f - 1 + 2 * upper
    at_end = (f == 0) | (f == n - 1)
    in_middle = (f > 0) & (f < n - 1)
    plane, core = t // 2, t % 2
    mate = t + 1 - 2 * core
    cross = (t + n // 2) % n
    leads = core == f % 2
    owner = f == t

    def near(c):
        return c + upper * (n - 1 - 2 * c)

    def far(c):
        return n - 1 - c + upper * (2 * c - n + 1)

    def rows_at(start, size):
        return pl.ds(start if isinstance(start, int) else pl.multiple_of(start, size), size)

    def side(h):
        return rows_at(h * half, half)

    small = [
        pltpu.make_async_copy(source, target, small_sem.at[i])
        for i, (source, target) in enumerate(
            (
                (tok_hbm, tok_ref), (gain_hbm, gain_ref), (post_hbm, post_ref),
                (cos_hbm, cos_ref), (sin_hbm, sin_ref),
            )
        )
    ]
    for fetch in small:
        fetch.start()
    fetches = []
    for g in range(kv):
        for ref, first, size in (
            (wq_hbm, 0, per * HEAD_DIM),
            (wk_hbm, per * HEAD_DIM, HEAD_DIM),
            (wv_hbm, (per + 1) * HEAD_DIM, HEAD_DIM),
        ):
            fetches.append(
                pltpu.make_async_copy(
                    ref.at[:, pl.ds(g * size, size)],
                    w_all.at[g, :, pl.ds(first, size)],
                    w_sem.at[len(fetches)],
                )
            )
    fetches.append(pltpu.make_async_copy(wo_hbm, wo, w_sem.at[len(fetches)]))
    for fetch in fetches:
        fetch.start()

    fetches = small[2:] + fetches
    held = pltpu.make_async_copy(tok_hbm, xs.at[f], held_sem)
    pl.when(owner)(lambda: held.start())
    for fetch in small[:2]:
        fetch.wait()
    tok = tok_ref[...].astype(jnp.float32)
    ss_got[f, t] = row_sums(tok * tok)[:1]
    pl.when(owner)(lambda: held.wait())
    finish_greeting()
    def is_outer(r):
        return (r == 0) | (r == n - 1)

    quarter, eighth = half // 2, half // 4
    away = jnp.logical_not(owner)
    detours = jnp.logical_not(is_outer(f)) & (plane != upper)
    relays = jnp.logical_not(is_outer(f)) & (plane == upper)

    def direct(h):
        return remote(
            tok_ref.at[side(h)], xs.at[f, side(h)], src_send.at[h], x_recv.at[f, h], t, t
        )

    def to_relay(h):
        return remote(
            tok_ref.at[side(h)], relay_buf.at[h], src_send.at[h], relay_recv.at[h], f, cross
        )

    def relayed(h):
        return remote(
            relay_buf.at[h], xs.at[f, side(h)], relay_send.at[h], x_recv.at[f, h], cross, t
        )

    def to_mate(r, h):
        spot = xs.at[r, side(h)]
        return remote(spot, spot, mate_send.at[r, h], x_recv.at[r, h], f, mate)

    def to_cross(r, h):
        spot = xs.at[r, side(h)]
        return remote(spot, spot, cross_send.at[r, h], x_recv.at[r, h], f, cross)

    def send_away(h):
        pl.when(away & jnp.logical_not(detours))(lambda: direct(h).start())
        pl.when(detours)(lambda: to_relay(h).start())

    def relay(h):
        @pl.when(relays)
        def _():
            to_relay(h).wait_recv()
            relayed(h).start()

    def total_out(a, b, c, d):
        row = ss_got.at[c, d]
        return remote(row, row, ss_send.at[a, b], ss_recv.at[c, d], a, b)

    def gain_out(k):
        return remote(
            gain_row, gain_row, gain_send.at[k - 1], gain_recv, f, (t + k) % n
        )

    def elsewhere(a, b):
        return jnp.logical_not((f == a) & (t == b))

    def start_totals():
        @pl.when(owner)
        def _():
            for i in range(lanes):
                cols = slice(i * 128, (i + 1) * 128)
                gain_row[:, cols] = gain_ref[cols].astype(jnp.float32)[None, :]
            for k in range(1, n):
                gain_out(k).start()

        for a in range(n):
            for b in range(n):
                pl.when(elsewhere(a, b))(lambda a=a, b=b: total_out(a, b, f, t).start())

    start_totals()

    def finish_totals():
        for r in range(n):
            for b in range(n):
                pl.when(elsewhere(r, b))(lambda r=r, b=b: total_out(r, b, r, b).wait_recv())
            total = ss_got[r, 0]
            for b in range(1, n):
                total = total + ss_got[r, b]
            scales[r] = lax.rsqrt(as_column(total) / total_width + eps_norm)
        pl.when(away)(lambda: gain_out(1).wait_recv())

    def normalise(r, h):
        def group(i):
            cols = rows_at(i * 128, 128)
            wide = xs[r, side(h), cols].astype(jnp.float32)
            xn[r, side(h), cols] = (
                wide * scales[r, side(h)] * gain_row[:, cols]
            ).astype(jnp.bfloat16)

        loop(0, lanes, group)

    def enters(r):
        by_owner = is_outer(r) | (r // 2 == upper)
        return leads & ((by_owner & owner) | jnp.logical_not(by_owner | owner))

    def spread(r, h, roles=(ENTRY, OTHER, LAST)):
        enter = enters(r)
        parts = {ENTRY: enter, OTHER: leads & jnp.logical_not(enter), LAST: jnp.logical_not(leads)}
        active = parts[roles[0]]
        for role in roles[1:]:
            active = active | parts[role]

        @pl.when(active & jnp.logical_not(owner & (r == f)))
        def _():
            to_mate(r, h).wait_recv()

        if ENTRY in roles:
            pl.when(enter)(lambda: to_cross(r, h).start())
        if roles != (LAST,):
            pl.when(active & leads)(lambda: to_mate(r, h).start())
        pl.when(active)(lambda: normalise(r, h))

    def place(k):
        j = k // kv
        return j // 2, j % 2, k % kv

    def partial(seq, h, g):
        return jnp.dot(xn[seq, side(h)], w_all[g], preferred_element_type=jnp.float32)

    def near_hop(k, recv):
        landing = near_got if recv is near_recv else far_got
        return remote(
            near_stage.at[k], landing.at[k], near_send.at[k], recv.at[k], inward, t
        )

    def far_hop(k):
        return remote(
            far_stage.at[k], far_got.at[k], far_send.at[k], far_recv.at[k], outward, t
        )

    def first_near(k):
        c, h, g = place(k)
        near_stage[k] = partial(near(c), h, g).astype(jnp.bfloat16)
        near_hop(k, near_recv).start()

    def middle_near(k):
        c, h, g = place(k)
        part = partial(near(c), h, g)
        near_hop(k, near_recv).wait_recv()
        near_stage[k] = (part + near_got[k].astype(jnp.float32)).astype(jnp.bfloat16)
        near_hop(k, far_recv).start()

    def middle_far(k):
        c, h, g = place(k)
        part = partial(far(c), h, g)
        far_hop(k).wait_recv()
        far_stage[k] = (part + far_got[k].astype(jnp.float32)).astype(jnp.bfloat16)
        far_hop(k).start()

    def share(s, h, g, there):
        return remote(
            att.at[s, g, side(h)], att.at[s, g, side(h)],
            att_send.at[s, h, g], att_recv.at[s, h, g], there, t,
        )

    def turn(u, span):
        other = pltpu.roll(u, HEAD_DIM // 2, 1)
        return (u * cos_ref[span] + other * sin_ref[span]).astype(jnp.bfloat16)

    def attend_piece(c, h, g):
        k = (c * 2 + h) * kv + g
        span, seen = slice(h * half, (h + 1) * half), (h + 1) * half
        part = partial(far(c), h, g)
        far_hop(k).wait_recv()
        raw = part + far_got[k].astype(jnp.float32)
        heads = [raw[:, i * HEAD_DIM : (i + 1) * HEAD_DIM] for i in range(per + 2)]
        keys[c, g, span] = turn(heads[per], span)
        values[c, g, span] = heads[per + 1].astype(jnp.bfloat16)
        query = jnp.concatenate([turn(u, span) for u in heads[:per]], axis=0)
        scores = lax.dot_general(
            query, keys[c, g, :seen], (((1,), (1,)), ((), ())),
            preferred_element_type=jnp.float32,
        )
        capped = soft_cap * jnp.tanh(scores * (attn_scale / soft_cap))
        index = lax.broadcasted_iota(jnp.int32, (half, seen), 0) + h * half
        allowed = lax.broadcasted_iota(jnp.int32, (half, seen), 1) <= index
        allowed = jnp.concatenate([allowed] * per, axis=0)
        e = jnp.where(allowed, jnp.exp(capped), 0.0)
        inverse = 1.0 / jnp.sum(e, axis=1, keepdims=True)
        probs = (e * inverse).astype(jnp.bfloat16)
        mixed = jnp.dot(probs, values[c, g, :seen], preferred_element_type=jnp.float32)
        for i in range(per):
            att[far(c), g, span, i * HEAD_DIM : (i + 1) * HEAD_DIM] = mixed[
                i * half : (i + 1) * half
            ].astype(jnp.bfloat16)
        share(far(c), h, g, inward).start()

    def part_hop(s, h):
        m = 2 * s + h
        return remote(
            part_stage.at[m, rows_at((1 - core) * quarter, quarter)], part_got.at[m],
            part_send.at[m], part_recv.at[m], f, mate,
        )

    def pair_hop(s, h):
        m = 2 * s + h
        return remote(
            pair_stage.at[m], pair_got.at[m], pair_send.at[m], pair_recv.at[m], f, cross
        )

    def sum_hop(s, h):
        m = 2 * s + h
        piece = core * 2 + plane
        return remote(
            sum_stage.at[m], proj.at[rows_at(h * half + piece * eighth, eighth)],
            sum_send.at[m], sum_recv.at[h, piece], s, f,
        )

    def pair_sum(m, which):
        kept = part_stage[m, rows_at(core * quarter + which * eighth, eighth)]
        got = part_got[m, rows_at(which * eighth, eighth)]
        return kept.astype(jnp.float32) + got.astype(jnp.float32)

    def out_first(s, h):
        m = 2 * s + h
        acc = jnp.dot(att[s, 0, side(h)], wo[: per * HEAD_DIM], preferred_element_type=jnp.float32)
        for g in range(1, kv):
            acc = acc + jnp.dot(
                att[s, g, side(h)],
                wo[g * per * HEAD_DIM : (g + 1) * per * HEAD_DIM],
                preferred_element_type=jnp.float32,
            )
        part_stage[m] = acc.astype(jnp.bfloat16)
        part_hop(s, h).start()

    def out_second(s, h):
        m = 2 * s + h
        part_hop(s, h).wait_recv()
        pair_stage[m] = pair_sum(m, 1 - plane).astype(jnp.bfloat16)
        pair_hop(s, h).start()

    def out_third(s, h):
        m = 2 * s + h
        pair_hop(s, h).wait_recv()
        summed = pair_sum(m, plane) + pair_got[m].astype(jnp.float32)
        stays = (s == f) & owner

        @pl.when(stays)
        def _():
            start = h * half + (core * 2 + plane) * eighth
            proj[rows_at(start, eighth)] = summed.astype(jnp.bfloat16)

        @pl.when(jnp.logical_not(stays))
        def _():
            sum_stage[m] = summed.astype(jnp.bfloat16)
            sum_hop(s, h).start()

    @pl.when(at_end)
    def _():
        def where(i):
            j = i % n
            c = j // 2
            return jnp.where(i < n, far(c), near(c)), j % 2

        send_away(0)

        @pl.when(owner)
        def _():
            for h in range(2):
                to_cross(f, h).start()
                to_mate(f, h).start()

        finish_totals()

        @pl.when(owner)
        def _():
            for h in range(2):
                normalise(f, h)

        for fetch in fetches[:-1]:
            fetch.wait()
        pl.when(owner)(lambda: to_cross(f, 0).wait_send())
        pl.when(away)(lambda: spread(near(0), 0))
        loop(0, EARLY, first_near)
        send_away(1)
        loop(EARLY, kv, first_near)
        pl.when(away)(lambda: spread(near(0), 1))
        loop(kv, 2 * kv, first_near)
        for h in range(2):
            spread(near(1), h)
            spread(far(0), h)
            loop((2 + h) * kv, (3 + h) * kv, first_near)
        for h in range(2):
            spread(far(1), h, (ENTRY,))
        fetches[-1].wait()

        def chunk(c):
            for h in range(2):
                pl.when(c == 1)(lambda h=h: spread(far(1), h, (OTHER, LAST)))
                loop(0, kv, lambda g: attend_piece(c, h, g))
                i = 2 * c + h
                out_first(*where(i))
                pl.when(i >= 1)(lambda: out_second(*where(i - 1)))

        loop(0, 2, chunk)

        out_second(*where(n - 1))

        def gather(i):
            s, h = where(i)
            for g in range(kv):
                share(s, h, g, inward).wait_recv()
            out_first(s, h)
            pl.when(i == n + HOLD)(lambda: loop(0, n, lambda j: out_third(*where(j))))
            out_second(s, h)
            out_third(s, h)

        loop(n, 2 * n, gather)

    @pl.when(in_middle)
    def _():
        def where(i):
            j = i // 2
            c = j // 2
            return jnp.where(i % 2 == 0, far(c), near(c)), j % 2

        for h in range(2):
            send_away(h)
        finish_totals()
        for fetch in fetches:
            fetch.wait()
        spread(near(0), 0)
        plan = (
            (far(0), 0, (0, 1, 2)), (near(0), 1, (2, 3, 4)), (far(0), 1, (2, 4, 5)),
            (near(1), 0, (1, 3, 5)), (far(1), 0, (2, 5, 8)),
            (near(1), 1, (3, 6, 8)), (far(1), 1, (3, 6, 10)),
        )

        def pass_on(k, seq, there):
            c, h, g = place(k)
            share(seq(c), h, g, there).wait_recv()
            share(seq(c), h, g, there).start()

        def step(s):
            for h in range(2):
                pl.when(s == h)(lambda h=h: relay(h))
            for seq, h, steps in plan:
                for role, at in enumerate(steps):
                    pl.when(s == at)(lambda seq=seq, h=h, role=role: spread(seq, h, (role,)))
            pl.when((s >= LAG) & (s < count + LAG))(lambda: middle_far(s - LAG))
            pl.when(s < count)(lambda: middle_near(s))
            late = jnp.maximum(s - FAR_RUSH, 0)
            for j in range(3):
                k = (s - FAR_AT) * 2 + late + j
                due = (s >= FAR_AT) & (k < count)
                if j == 2:
                    due = due & (s >= FAR_RUSH)
                pl.when(due)(lambda k=k: pass_on(k, far, inward))
            m = s - OUT_AT
            pl.when(m >= 1)(lambda: out_second(*where(m - 1)))
            for j in range(NEAR_PACE):
                k = (s - NEAR_AT) * NEAR_PACE + j
                pl.when((k >= 0) & (k < count))(lambda k=k: pass_on(k, near, outward))
            pl.when(m >= 0)(lambda: out_first(*where(m)))

        loop(0, OUT_AT + 2 * n, step)
        loop(0, 2 * n - 1, lambda i: out_third(*where(i)))
        out_second(*where(2 * n - 1))
        out_third(*where(2 * n - 1))

    def post_out(h, k, slot):
        return remote(
            post_mine.at[h], post_got.at[h, slot],
            post_send.at[h, k - 1], post_recv.at[h, slot], f, (t + k) % n,
        )

    for h in range(2):
        for piece in range(n):
            mine = owner & (core * 2 + plane == piece)

            @pl.when(jnp.logical_not(mine))
            def _():
                spot = proj.at[rows_at(h * half + piece * eighth, eighth)]
                remote(
                    spot, spot, sum_send.at[0], sum_recv.at[h, piece], f, t
                ).wait_recv()

        branch = proj[side(h)].astype(jnp.float32)
        post_mine[h] = row_sums(branch * branch)
        for k in range(1, n):
            post_out(h, k, t).start()
    for h in range(2):
        total = post_mine[h]
        for k in range(1, n):
            slot = (t + k) % n
            post_out(h, k, slot).wait_recv()
            total = total + post_got[h, slot]
        scale = lax.rsqrt(as_column(total) / total_width + eps_norm)
        for i in range(lanes):
            cols = slice(i * 128, (i + 1) * 128)
            out_ref[side(h), cols] = tok_ref[side(h), cols].astype(jnp.float32) + (
                proj[side(h), cols].astype(jnp.float32) * scale * post_ref[cols].astype(jnp.float32)[None, :]
            )

    for a in range(n):
        for b in range(n):
            pl.when(elsewhere(a, b))(lambda: total_out(a, b, f, t).wait_send())
    for k in range(1, n):
        pl.when(owner)(lambda: gain_out(k).wait_send())
        for h in range(2):
            post_out(h, k, t).wait_send()

    for h in range(2):
        pl.when(away)(lambda: direct(h).wait_send())
        pl.when(relays)(lambda: relayed(h).wait_send())

    def drain(r):
        for h in range(2):
            waited = owner & (r == f) & is_outer(r) & (h == 0)
            pl.when(enters(r) & jnp.logical_not(waited))(lambda: to_cross(r, h).wait_send())
            pl.when(leads)(lambda: to_mate(r, h).wait_send())

        for h in range(2):
            part_hop(r, h).wait_send()
            pair_hop(r, h).wait_send()
            pl.when(jnp.logical_not((r == f) & owner))(lambda: sum_hop(r, h).wait_send())
            sent = in_middle | (r == far(0)) | (r == far(1))

            @pl.when(sent)
            def _():
                for g in range(kv):
                    share(r, h, g, inward).wait_send()

    loop(0, n, drain)

    def drain_hops(k):
        near_hop(k, far_recv).wait_send()
        pl.when(in_middle)(lambda: far_hop(k).wait_send())

    loop(0, count, drain_hops)


def whole_block(n, tokens, gain, post_gain, cosine, sine, w_query, w_key, w_value, w_out):
    rows, width = tokens.shape
    half, kv = rows // 2, w_key.shape[1] // HEAD_DIM
    per = w_query.shape[1] // w_key.shape[1]
    wide = (per + 2) * HEAD_DIM
    count = 4 * kv
    dma = pltpu.SemaphoreType.DMA
    bf16 = lambda *shape: pltpu.VMEM(shape, jnp.bfloat16)
    f32 = lambda *shape: pltpu.VMEM(shape, jnp.float32)
    vmem = pl.BlockSpec(memory_space=pltpu.VMEM)
    in_hbm = pl.BlockSpec(memory_space=pltpu.HBM)
    return pl.pallas_call(
        functools.partial(block_kernel, n),
        out_shape=pltpu.VMEM((rows, width), jnp.float32),
        in_specs=[in_hbm] * 9,
        out_specs=vmem,
        scratch_shapes=[
            bf16(rows, width), bf16(width), bf16(width), f32(rows, HEAD_DIM), f32(rows, HEAD_DIM),
            dma((5,)),
            bf16(kv, width, wide), bf16(*w_out.shape), bf16(n, rows, width),
            bf16(n, rows, width), bf16(2, half, width), f32(n, n, 1, rows),
            f32(n, rows, 128), f32(1, width),
            bf16(count, half, wide), bf16(count, half, wide),
            bf16(count, half, wide), bf16(count, half, wide),
            bf16(2, kv, rows, HEAD_DIM), bf16(2, kv, rows, HEAD_DIM),
            bf16(n, kv, rows, per * HEAD_DIM),
            bf16(2 * n, half, width), bf16(2 * n, half // 2, width),
            bf16(2 * n, half // 4, width), bf16(2 * n, half // 4, width),
            bf16(2 * n, half // 4, width), bf16(rows, width),
            f32(2, 8, half), f32(2, n, 8, half),
            dma((3 * kv + 1,)), dma(()), dma((n - 1,)), dma(()), dma((n, n)), dma((n, n)), dma((2,)), dma((2,)), dma((2,)),
            dma((n, 2)), dma((n, 2)), dma((n, 2)),
            dma((count,)), dma((count,)), dma((count,)), dma((count,)),
            dma((n, 2, kv)), dma((n, 2, kv)),
            dma((2 * n,)), dma((2 * n,)), dma((2 * n,)), dma((2 * n,)),
            dma((2 * n,)), dma((2, n)),
            dma((2, n - 1)), dma((2, n)),
        ],
        compiler_params=pltpu.CompilerParams(
            collective_id=0, has_side_effects=True, vmem_limit_bytes=VMEM_LIMIT
        ),
    )(tokens, gain, post_gain, cosine, sine, w_query, w_key, w_value, w_out)


def tables(rows):
    half = HEAD_DIM // 2
    freq = np.float32(rope_base) ** (-(np.arange(half, dtype=np.float32) * np.float32(2.0 / HEAD_DIM)))
    angle = np.arange(rows, dtype=np.float32)[:, None] * freq[None, :].astype(np.float32)
    cosine, sine = np.cos(angle), np.sin(angle)
    return (
        jnp.asarray(np.concatenate([cosine, cosine], axis=1), jnp.float32),
        jnp.asarray(np.concatenate([-sine, sine], axis=1), jnp.float32),
    )


def solution(mesh):
    n_fsdp, n_tensor = mesh.shape["fsdp"], mesh.shape["tensor"]

    def on_device(tokens, norm_gain, w_query, w_key, w_value, w_out, post_gain):
        rows = tokens.shape[0]
        width = tokens.shape[1] * n_tensor
        if n_fsdp == n_tensor == CHAIN:
            return whole_block(
                n_fsdp, tokens, norm_gain, post_gain, *tables(rows), w_query, w_key, w_value, w_out
            )
        widened = tokens.astype(jnp.float32)
        total = lax.psum(jnp.sum(widened * widened, axis=1), "tensor")
        normed = (
            widened * lax.rsqrt(total / width + eps_norm)[:, None] * norm_gain.astype(jnp.float32)
        ).astype(jnp.bfloat16)
        mine = to_rows(normed, n_fsdp, n_tensor)
        raw = []
        for piece in (w_query, w_key, w_value):
            part = jnp.dot(mine, piece, preferred_element_type=jnp.float32).astype(jnp.bfloat16)
            parts = lax.all_to_all(part, "fsdp", 0, 0, tiled=True)
            parts = parts.reshape(n_fsdp, rows, piece.shape[1])
            raw.append(jnp.sum(parts.astype(jnp.float32), axis=0))
        query_raw, key_raw, value_raw = raw
        position = jnp.arange(rows, dtype=jnp.int32)
        local_heads = w_query.shape[1] // HEAD_DIM
        local_kv = w_key.shape[1] // HEAD_DIM
        query = rotate(query_raw.reshape(rows, local_heads, HEAD_DIM), position)
        key = rotate(key_raw.reshape(rows, local_kv, HEAD_DIM), position)
        query, key = query.astype(jnp.bfloat16), key.astype(jnp.bfloat16)
        value = value_raw.astype(jnp.bfloat16).reshape(rows, local_kv, HEAD_DIM)
        attn = attend(query, key, value, position)
        attn_all = lax.all_gather(attn, "fsdp", axis=0, tiled=True)
        part = jnp.dot(attn_all, w_out, preferred_element_type=jnp.float32).astype(jnp.bfloat16)
        summed = lax.psum_scatter(part, "tensor", scatter_dimension=0, tiled=True)
        proj = from_rows(summed, rows, n_fsdp, n_tensor).astype(jnp.float32)
        post_total = lax.psum(jnp.sum(proj * proj, axis=1), "tensor")
        branch = (
            proj
            * lax.rsqrt(post_total / width + eps_norm)[:, None]
            * post_gain.astype(jnp.float32)
        )
        return tokens.astype(jnp.float32) + branch

    placed = (
        P(("groups", "fsdp"), "tensor"),
        P("tensor"),
        P("fsdp", "tensor"),
        P("fsdp", "tensor"),
        P("fsdp", "tensor"),
        P("tensor", "fsdp"),
        P("tensor"),
    )
    return jax.shard_map(
        on_device,
        mesh=mesh,
        in_specs=placed,
        out_specs=P(("groups", "fsdp"), "tensor"),
        check_vma=False,
    )
```

```python
import functools

import jax
import numpy as np
import jax.numpy as jnp
from jax import lax
from jax.experimental import pallas as pl
from jax.experimental.pallas import tpu as pltpu
from jax.sharding import PartitionSpec as P

HEAD_DIM = 128

eps_norm = 1e-06
soft_cap = 50.0
attn_scale = 144.0 ** (-0.5)
rope_base = 10000.0


def rotate(values, position):
    head_dim = values.shape[-1]
    half = head_dim // 2
    freq = rope_base ** (-(jnp.arange(half, dtype=jnp.float32) * 2.0 / head_dim))
    angle = position.astype(jnp.float32)[:, None] * freq[None, :]
    cosine = jnp.cos(angle)[:, None, :]
    sine = jnp.sin(angle)[:, None, :]
    first = values[..., :half]
    second = values[..., half:]
    return jnp.concatenate(
        [first * cosine - second * sine, second * cosine + first * sine], axis=-1
    )


def attend(query, keys, values, position):
    count, heads, head_dim = query.shape
    kv_count = keys.shape[1]
    grouped = query.reshape(count, kv_count, heads // kv_count, head_dim)
    scores = (
        jnp.einsum("nkgd,mkd->kgnm", grouped, keys, preferred_element_type=jnp.float32) * attn_scale
    )
    capped = soft_cap * jnp.tanh(scores / soft_cap)
    allowed = position[None, :] <= position[:, None]
    weights = jnp.where(allowed, jnp.exp(capped), 0.0)
    probs = (weights / jnp.sum(weights, axis=-1, keepdims=True)).astype(jnp.bfloat16)
    mixed = jnp.einsum("kgnm,mkd->nkgd", probs, values, preferred_element_type=jnp.float32)
    return mixed.reshape(count, heads * head_dim).astype(jnp.bfloat16)


def swap_pairs(n_fsdp, n_tensor, turn):
    ratio = n_fsdp // n_tensor
    pairs = []
    for f in range(n_fsdp):
        for t in range(n_tensor):
            j = (f + turn) % ratio
            pairs.append((f * n_tensor + t, (t * ratio + j) * n_tensor + f // ratio))
    return pairs


def to_rows(block, n_fsdp, n_tensor):
    rows = block.shape[0]
    ratio = n_fsdp // n_tensor
    width = block.shape[1] // ratio
    f = lax.axis_index("fsdp")
    if ratio == 1:
        held = lax.ppermute(block, ("fsdp", "tensor"), swap_pairs(n_fsdp, n_tensor, 0))
    else:
        held = jnp.zeros((ratio, rows, width), block.dtype)
        for turn in range(ratio):
            piece = lax.dynamic_slice_in_dim(block, (f + turn) % ratio * width, width, 1)
            got = lax.ppermute(piece, ("fsdp", "tensor"), swap_pairs(n_fsdp, n_tensor, turn))
            held = lax.dynamic_update_index_in_dim(held, got, (f - turn) % ratio, 0)
        held = held.reshape(ratio * rows, width)
    return lax.all_gather(held, "tensor", axis=0, tiled=True)


def from_rows(summed, rows, n_fsdp, n_tensor):
    ratio = n_fsdp // n_tensor
    width = summed.shape[1]
    f = lax.axis_index("fsdp")
    back = lambda turn: [(b, a) for a, b in swap_pairs(n_fsdp, n_tensor, turn)]
    if ratio == 1:
        return lax.ppermute(summed, ("fsdp", "tensor"), back(0))
    pieces = summed.reshape(ratio, rows, width)
    out = jnp.zeros((rows, ratio * width), summed.dtype)
    for turn in range(ratio):
        piece = lax.dynamic_index_in_dim(pieces, (f - turn) % ratio, 0, keepdims=False)
        got = lax.ppermute(piece, ("fsdp", "tensor"), back(turn))
        out = lax.dynamic_update_slice_in_dim(out, got, (f + turn) % ratio * width, 1)
    return out


MESH = pl.DeviceIdType.MESH
VMEM_LIMIT = 60 * 1024 * 1024
CHAIN = 4
LAG = 3
FAR_AT, FAR_RUSH = 15, 18
NEAR_AT, NEAR_PACE = 17, 2
OUT_AT = 17
EARLY = 3
HOLD = 3
ENTRY, OTHER, LAST = 0, 1, 2


def remote(src, dst, send, recv, a, b):
    return pltpu.make_async_remote_copy(
        src_ref=src,
        dst_ref=dst,
        send_sem=send,
        recv_sem=recv,
        device_id={"fsdp": a, "tensor": b},
        device_id_type=MESH,
    )


def greet(n, f, t):
    barrier = pltpu.get_barrier_semaphore()
    for a in range(n):
        for b in range(n):
            @pl.when(jnp.logical_not((f == a) & (t == b)))
            def _():
                pl.semaphore_signal(
                    barrier, inc=1, device_id={"fsdp": a, "tensor": b}, device_id_type=MESH
                )
    return lambda: pl.semaphore_wait(barrier, n * n - 1)


def loop(low, high, body):
    def step(i, carry):
        body(i)
        return carry

    lax.fori_loop(low, high, step, 0)


def row_sums(squares):
    groups = squares.shape[1] // 128
    lanes = squares[:, :128]
    for i in range(1, groups):
        lanes = lanes + squares[:, i * 128 : (i + 1) * 128]
    row = jnp.sum(lanes.T, axis=0, keepdims=True)
    return jnp.broadcast_to(row, (8, squares.shape[0]))


def as_column(row):
    return jnp.broadcast_to(row[:1], (128, row.shape[1])).T


def block_kernel(
    n, tok_hbm, gain_hbm, post_hbm, cos_hbm, sin_hbm, wq_hbm, wk_hbm, wv_hbm, wo_hbm, out_ref,
    tok_ref, gain_ref, post_ref, cos_ref, sin_ref, small_sem, w_all, wo, xn, xs, relay_buf, ss_got, scales, gain_row,
    near_stage, far_stage, near_got, far_got, keys, values, att,
    part_stage, part_got, pair_stage, pair_got, sum_stage, proj, post_mine, post_got,
    w_sem, held_sem, gain_send, gain_recv, ss_send, ss_recv, src_send, relay_recv, relay_send,
    x_recv, mate_send, cross_send, near_send, near_recv, far_send, far_recv,
    att_send, att_recv, part_send, part_recv, pair_send, pair_recv, sum_send, sum_recv,
    post_send, post_recv,
):
    f, t = lax.axis_index("fsdp"), lax.axis_index("tensor")
    rows, width = tok_ref.shape
    half = rows // 2
    kv = w_all.shape[0]
    per = att.shape[3] // HEAD_DIM
    count = 4 * kv
    lanes = width // 128
    total_width = width * n
    finish_greeting = greet(n, f, t)

    upper = f // 2
    inward = f + 1 - 2 * upper
    outward = f - 1 + 2 * upper
    at_end = (f == 0) | (f == n - 1)
    in_middle = (f > 0) & (f < n - 1)
    plane, core = t // 2, t % 2
    mate = t + 1 - 2 * core
    cross = (t + n // 2) % n
    leads = core == f % 2
    owner = f == t

    def near(c):
        return c + upper * (n - 1 - 2 * c)

    def far(c):
        return n - 1 - c + upper * (2 * c - n + 1)

    def rows_at(start, size):
        return pl.ds(start if isinstance(start, int) else pl.multiple_of(start, size), size)

    def side(h):
        return rows_at(h * half, half)

    small = [
        pltpu.make_async_copy(source, target, small_sem.at[i])
        for i, (source, target) in enumerate(
            (
                (tok_hbm, tok_ref), (gain_hbm, gain_ref), (post_hbm, post_ref),
                (cos_hbm, cos_ref), (sin_hbm, sin_ref),
            )
        )
    ]
    for fetch in small:
        fetch.start()
    fetches = []
    for g in range(kv):
        for ref, first, size in (
            (wq_hbm, 0, per * HEAD_DIM),
            (wk_hbm, per * HEAD_DIM, HEAD_DIM),
            (wv_hbm, (per + 1) * HEAD_DIM, HEAD_DIM),
        ):
            fetches.append(
                pltpu.make_async_copy(
                    ref.at[:, pl.ds(g * size, size)],
                    w_all.at[g, :, pl.ds(first, size)],
                    w_sem.at[len(fetches)],
                )
            )
    fetches.append(pltpu.make_async_copy(wo_hbm, wo, w_sem.at[len(fetches)]))
    for fetch in fetches:
        fetch.start()

    fetches = small[2:] + fetches
    held = pltpu.make_async_copy(tok_hbm, xs.at[f], held_sem)
    pl.when(owner)(lambda: held.start())
    for fetch in small[:2]:
        fetch.wait()
    tok = tok_ref[...].astype(jnp.float32)
    ss_got[f, t] = row_sums(tok * tok)[:1]
    pl.when(owner)(lambda: held.wait())
    finish_greeting()
    def is_outer(r):
        return (r == 0) | (r == n - 1)

    quarter, eighth = half // 2, half // 4
    away = jnp.logical_not(owner)
    detours = jnp.logical_not(is_outer(f)) & (plane != upper)
    relays = jnp.logical_not(is_outer(f)) & (plane == upper)

    def direct(h):
        return remote(
            tok_ref.at[side(h)], xs.at[f, side(h)], src_send.at[h], x_recv.at[f, h], t, t
        )

    def to_relay(h):
        return remote(
            tok_ref.at[side(h)], relay_buf.at[h], src_send.at[h], relay_recv.at[h], f, cross
        )

    def relayed(h):
        return remote(
            relay_buf.at[h], xs.at[f, side(h)], relay_send.at[h], x_recv.at[f, h], cross, t
        )

    def to_mate(r, h):
        spot = xs.at[r, side(h)]
        return remote(spot, spot, mate_send.at[r, h], x_recv.at[r, h], f, mate)

    def to_cross(r, h):
        spot = xs.at[r, side(h)]
        return remote(spot, spot, cross_send.at[r, h], x_recv.at[r, h], f, cross)

    def send_away(h):
        pl.when(away & jnp.logical_not(detours))(lambda: direct(h).start())
        pl.when(detours)(lambda: to_relay(h).start())

    def relay(h):
        @pl.when(relays)
        def _():
            to_relay(h).wait_recv()
            relayed(h).start()

    def total_out(a, b, c, d):
        row = ss_got.at[c, d]
        return remote(row, row, ss_send.at[a, b], ss_recv.at[c, d], a, b)

    def gain_out(k):
        return remote(
            gain_row, gain_row, gain_send.at[k - 1], gain_recv, f, (t + k) % n
        )

    def elsewhere(a, b):
        return jnp.logical_not((f == a) & (t == b))

    def start_totals():
        @pl.when(owner)
        def _():
            for i in range(lanes):
                cols = slice(i * 128, (i + 1) * 128)
                gain_row[:, cols] = gain_ref[cols].astype(jnp.float32)[None, :]
            for k in range(1, n):
                gain_out(k).start()

        for a in range(n):
            for b in range(n):
                pl.when(elsewhere(a, b))(lambda a=a, b=b: total_out(a, b, f, t).start())

    start_totals()

    def finish_totals():
        for r in range(n):
            for b in range(n):
                pl.when(elsewhere(r, b))(lambda r=r, b=b: total_out(r, b, r, b).wait_recv())
            total = ss_got[r, 0]
            for b in range(1, n):
                total = total + ss_got[r, b]
            scales[r] = lax.rsqrt(as_column(total) / total_width + eps_norm)
        pl.when(away)(lambda: gain_out(1).wait_recv())

    def normalise(r, h):
        def group(i):
            cols = rows_at(i * 128, 128)
            wide = xs[r, side(h), cols].astype(jnp.float32)
            xn[r, side(h), cols] = (
                wide * scales[r, side(h)] * gain_row[:, cols]
            ).astype(jnp.bfloat16)

        loop(0, lanes, group)

    def enters(r):
        by_owner = is_outer(r) | (r // 2 == upper)
        return leads & ((by_owner & owner) | jnp.logical_not(by_owner | owner))

    def spread(r, h, roles=(ENTRY, OTHER, LAST)):
        enter = enters(r)
        parts = {ENTRY: enter, OTHER: leads & jnp.logical_not(enter), LAST: jnp.logical_not(leads)}
        active = parts[roles[0]]
        for role in roles[1:]:
            active = active | parts[role]

        @pl.when(active & jnp.logical_not(owner & (r == f)))
        def _():
            to_mate(r, h).wait_recv()

        if ENTRY in roles:
            pl.when(enter)(lambda: to_cross(r, h).start())
        if roles != (LAST,):
            pl.when(active & leads)(lambda: to_mate(r, h).start())
        pl.when(active)(lambda: normalise(r, h))

    def place(k):
        j = k // kv
        return j // 2, j % 2, k % kv

    def partial(seq, h, g):
        return jnp.dot(xn[seq, side(h)], w_all[g], preferred_element_type=jnp.float32)

    def near_hop(k, recv):
        landing = near_got if recv is near_recv else far_got
        return remote(
            near_stage.at[k], landing.at[k], near_send.at[k], recv.at[k], inward, t
        )

    def far_hop(k):
        return remote(
            far_stage.at[k], far_got.at[k], far_send.at[k], far_recv.at[k], outward, t
        )

    def first_near(k):
        c, h, g = place(k)
        near_stage[k] = partial(near(c), h, g).astype(jnp.bfloat16)
        near_hop(k, near_recv).start()

    def middle_near(k):
        c, h, g = place(k)
        part = partial(near(c), h, g)
        near_hop(k, near_recv).wait_recv()
        near_stage[k] = (part + near_got[k].astype(jnp.float32)).astype(jnp.bfloat16)
        near_hop(k, far_recv).start()

    def middle_far(k):
        c, h, g = place(k)
        part = partial(far(c), h, g)
        far_hop(k).wait_recv()
        far_stage[k] = (part + far_got[k].astype(jnp.float32)).astype(jnp.bfloat16)
        far_hop(k).start()

    def share(s, h, g, there):
        return remote(
            att.at[s, g, side(h)], att.at[s, g, side(h)],
            att_send.at[s, h, g], att_recv.at[s, h, g], there, t,
        )

    def turn(u, span):
        other = pltpu.roll(u, HEAD_DIM // 2, 1)
        return (u * cos_ref[span] + other * sin_ref[span]).astype(jnp.bfloat16)

    def attend_piece(c, h, g):
        k = (c * 2 + h) * kv + g
        span, seen = slice(h * half, (h + 1) * half), (h + 1) * half
        part = partial(far(c), h, g)
        far_hop(k).wait_recv()
        raw = part + far_got[k].astype(jnp.float32)
        heads = [raw[:, i * HEAD_DIM : (i + 1) * HEAD_DIM] for i in range(per + 2)]
        keys[c, g, span] = turn(heads[per], span)
        values[c, g, span] = heads[per + 1].astype(jnp.bfloat16)
        query = jnp.concatenate([turn(u, span) for u in heads[:per]], axis=0)
        scores = lax.dot_general(
            query, keys[c, g, :seen], (((1,), (1,)), ((), ())),
            preferred_element_type=jnp.float32,
        )
        capped = soft_cap * jnp.tanh(scores * (attn_scale / soft_cap))
        index = lax.broadcasted_iota(jnp.int32, (half, seen), 0) + h * half
        allowed = lax.broadcasted_iota(jnp.int32, (half, seen), 1) <= index
        allowed = jnp.concatenate([allowed] * per, axis=0)
        e = jnp.where(allowed, jnp.exp(capped), 0.0)
        inverse = 1.0 / jnp.sum(e, axis=1, keepdims=True)
        probs = (e * inverse).astype(jnp.bfloat16)
        mixed = jnp.dot(probs, values[c, g, :seen], preferred_element_type=jnp.float32)
        for i in range(per):
            att[far(c), g, span, i * HEAD_DIM : (i + 1) * HEAD_DIM] = mixed[
                i * half : (i + 1) * half
            ].astype(jnp.bfloat16)
        share(far(c), h, g, inward).start()

    def part_hop(s, h):
        m = 2 * s + h
        return remote(
            part_stage.at[m, rows_at((1 - core) * quarter, quarter)], part_got.at[m],
            part_send.at[m], part_recv.at[m], f, mate,
        )

    def pair_hop(s, h):
        m = 2 * s + h
        return remote(
            pair_stage.at[m], pair_got.at[m], pair_send.at[m], pair_recv.at[m], f, cross
        )

    def sum_hop(s, h):
        m = 2 * s + h
        piece = core * 2 + plane
        return remote(
            sum_stage.at[m], proj.at[rows_at(h * half + piece * eighth, eighth)],
            sum_send.at[m], sum_recv.at[h, piece], s, f,
        )

    def pair_sum(m, which):
        kept = part_stage[m, rows_at(core * quarter + which * eighth, eighth)]
        got = part_got[m, rows_at(which * eighth, eighth)]
        return kept.astype(jnp.float32) + got.astype(jnp.float32)

    def out_first(s, h):
        m = 2 * s + h
        acc = jnp.dot(att[s, 0, side(h)], wo[: per * HEAD_DIM], preferred_element_type=jnp.float32)
        for g in range(1, kv):
            acc = acc + jnp.dot(
                att[s, g, side(h)],
                wo[g * per * HEAD_DIM : (g + 1) * per * HEAD_DIM],
                preferred_element_type=jnp.float32,
            )
        part_stage[m] = acc.astype(jnp.bfloat16)
        part_hop(s, h).start()

    def out_second(s, h):
        m = 2 * s + h
        part_hop(s, h).wait_recv()
        pair_stage[m] = pair_sum(m, 1 - plane).astype(jnp.bfloat16)
        pair_hop(s, h).start()

    def out_third(s, h):
        m = 2 * s + h
        pair_hop(s, h).wait_recv()
        summed = pair_sum(m, plane) + pair_got[m].astype(jnp.float32)
        stays = (s == f) & owner

        @pl.when(stays)
        def _():
            start = h * half + (core * 2 + plane) * eighth
            proj[rows_at(start, eighth)] = summed.astype(jnp.bfloat16)

        @pl.when(jnp.logical_not(stays))
        def _():
            sum_stage[m] = summed.astype(jnp.bfloat16)
            sum_hop(s, h).start()

    @pl.when(at_end)
    def _():
        def where(i):
            j = i % n
            c = j // 2
            return jnp.where(i < n, far(c), near(c)), j % 2

        send_away(0)

        @pl.when(owner)
        def _():
            for h in range(2):
                to_cross(f, h).start()
                to_mate(f, h).start()

        finish_totals()

        @pl.when(owner)
        def _():
            for h in range(2):
                normalise(f, h)

        for fetch in fetches[:-1]:
            fetch.wait()
        pl.when(owner)(lambda: to_cross(f, 0).wait_send())
        pl.when(away)(lambda: spread(near(0), 0))
        loop(0, EARLY, first_near)
        send_away(1)
        loop(EARLY, kv, first_near)
        pl.when(away)(lambda: spread(near(0), 1))
        loop(kv, 2 * kv, first_near)
        for h in range(2):
            spread(near(1), h)
            spread(far(0), h)
            loop((2 + h) * kv, (3 + h) * kv, first_near)
        for h in range(2):
            spread(far(1), h, (ENTRY,))
        fetches[-1].wait()

        def chunk(c):
            for h in range(2):
                pl.when(c == 1)(lambda h=h: spread(far(1), h, (OTHER, LAST)))
                loop(0, kv, lambda g: attend_piece(c, h, g))
                i = 2 * c + h
                out_first(*where(i))
                pl.when(i >= 1)(lambda: out_second(*where(i - 1)))

        loop(0, 2, chunk)

        out_second(*where(n - 1))

        def gather(i):
            s, h = where(i)
            for g in range(kv):
                share(s, h, g, inward).wait_recv()
            out_first(s, h)
            pl.when(i == n + HOLD)(lambda: loop(0, n, lambda j: out_third(*where(j))))
            out_second(s, h)
            out_third(s, h)

        loop(n, 2 * n, gather)

    @pl.when(in_middle)
    def _():
        def where(i):
            j = i // 2
            c = j // 2
            return jnp.where(i % 2 == 0, far(c), near(c)), j % 2

        for h in range(2):
            send_away(h)
        finish_totals()
        for fetch in fetches:
            fetch.wait()
        spread(near(0), 0)
        plan = (
            (far(0), 0, (0, 1, 2)), (near(0), 1, (2, 3, 4)), (far(0), 1, (2, 4, 5)),
            (near(1), 0, (1, 3, 5)), (far(1), 0, (2, 5, 8)),
            (near(1), 1, (3, 6, 8)), (far(1), 1, (3, 6, 10)),
        )

        def pass_on(k, seq, there):
            c, h, g = place(k)
            share(seq(c), h, g, there).wait_recv()
            share(seq(c), h, g, there).start()

        def step(s):
            for h in range(2):
                pl.when(s == h)(lambda h=h: relay(h))
            for seq, h, steps in plan:
                for role, at in enumerate(steps):
                    pl.when(s == at)(lambda seq=seq, h=h, role=role: spread(seq, h, (role,)))
            pl.when((s >= LAG) & (s < count + LAG))(lambda: middle_far(s - LAG))
            pl.when(s < count)(lambda: middle_near(s))
            late = jnp.maximum(s - FAR_RUSH, 0)
            for j in range(3):
                k = (s - FAR_AT) * 2 + late + j
                due = (s >= FAR_AT) & (k < count)
                if j == 2:
                    due = due & (s >= FAR_RUSH)
                pl.when(due)(lambda k=k: pass_on(k, far, inward))
            m = s - OUT_AT
            pl.when(m >= 1)(lambda: out_second(*where(m - 1)))
            for j in range(NEAR_PACE):
                k = (s - NEAR_AT) * NEAR_PACE + j
                pl.when((k >= 0) & (k < count))(lambda k=k: pass_on(k, near, outward))
            pl.when(m >= 0)(lambda: out_first(*where(m)))

        loop(0, OUT_AT + 2 * n, step)
        loop(0, 2 * n - 1, lambda i: out_third(*where(i)))
        out_second(*where(2 * n - 1))
        out_third(*where(2 * n - 1))

    def post_out(h, k, slot):
        return remote(
            post_mine.at[h], post_got.at[h, slot],
            post_send.at[h, k - 1], post_recv.at[h, slot], f, (t + k) % n,
        )

    for h in range(2):
        for piece in range(n):
            mine = owner & (core * 2 + plane == piece)

            @pl.when(jnp.logical_not(mine))
            def _():
                spot = proj.at[rows_at(h * half + piece * eighth, eighth)]
                remote(
                    spot, spot, sum_send.at[0], sum_recv.at[h, piece], f, t
                ).wait_recv()

        branch = proj[side(h)].astype(jnp.float32)
        post_mine[h] = row_sums(branch * branch)
        for k in range(1, n):
            post_out(h, k, t).start()
    for h in range(2):
        total = post_mine[h]
        for k in range(1, n):
            slot = (t + k) % n
            post_out(h, k, slot).wait_recv()
            total = total + post_got[h, slot]
        scale = lax.rsqrt(as_column(total) / total_width + eps_norm)
        for i in range(lanes):
            cols = slice(i * 128, (i + 1) * 128)
            out_ref[side(h), cols] = tok_ref[side(h), cols].astype(jnp.float32) + (
                proj[side(h), cols].astype(jnp.float32) * scale * post_ref[cols].astype(jnp.float32)[None, :]
            )

    for a in range(n):
        for b in range(n):
            pl.when(elsewhere(a, b))(lambda: total_out(a, b, f, t).wait_send())
    for k in range(1, n):
        pl.when(owner)(lambda: gain_out(k).wait_send())
        for h in range(2):
            post_out(h, k, t).wait_send()

    for h in range(2):
        pl.when(away)(lambda: direct(h).wait_send())
        pl.when(relays)(lambda: relayed(h).wait_send())

    def drain(r):
        for h in range(2):
            waited = owner & (r == f) & is_outer(r) & (h == 0)
            pl.when(enters(r) & jnp.logical_not(waited))(lambda: to_cross(r, h).wait_send())
            pl.when(leads)(lambda: to_mate(r, h).wait_send())

        for h in range(2):
            part_hop(r, h).wait_send()
            pair_hop(r, h).wait_send()
            pl.when(jnp.logical_not((r == f) & owner))(lambda: sum_hop(r, h).wait_send())
            sent = in_middle | (r == far(0)) | (r == far(1))

            @pl.when(sent)
            def _():
                for g in range(kv):
                    share(r, h, g, inward).wait_send()

    loop(0, n, drain)

    def drain_hops(k):
        near_hop(k, far_recv).wait_send()
        pl.when(in_middle)(lambda: far_hop(k).wait_send())

    loop(0, count, drain_hops)


def whole_block(n, tokens, gain, post_gain, cosine, sine, w_query, w_key, w_value, w_out):
    rows, width = tokens.shape
    half, kv = rows // 2, w_key.shape[1] // HEAD_DIM
    per = w_query.shape[1] // w_key.shape[1]
    wide = (per + 2) * HEAD_DIM
    count = 4 * kv
    dma = pltpu.SemaphoreType.DMA
    bf16 = lambda *shape: pltpu.VMEM(shape, jnp.bfloat16)
    f32 = lambda *shape: pltpu.VMEM(shape, jnp.float32)
    vmem = pl.BlockSpec(memory_space=pltpu.VMEM)
    in_hbm = pl.BlockSpec(memory_space=pltpu.HBM)
    return pl.pallas_call(
        functools.partial(block_kernel, n),
        out_shape=pltpu.VMEM((rows, width), jnp.float32),
        in_specs=[in_hbm] * 9,
        out_specs=vmem,
        scratch_shapes=[
            bf16(rows, width), bf16(width), bf16(width), f32(rows, HEAD_DIM), f32(rows, HEAD_DIM),
            dma((5,)),
            bf16(kv, width, wide), bf16(*w_out.shape), bf16(n, rows, width),
            bf16(n, rows, width), bf16(2, half, width), f32(n, n, 1, rows),
            f32(n, rows, 128), f32(1, width),
            bf16(count, half, wide), bf16(count, half, wide),
            bf16(count, half, wide), bf16(count, half, wide),
            bf16(2, kv, rows, HEAD_DIM), bf16(2, kv, rows, HEAD_DIM),
            bf16(n, kv, rows, per * HEAD_DIM),
            bf16(2 * n, half, width), bf16(2 * n, half // 2, width),
            bf16(2 * n, half // 4, width), bf16(2 * n, half // 4, width),
            bf16(2 * n, half // 4, width), bf16(rows, width),
            f32(2, 8, half), f32(2, n, 8, half),
            dma((3 * kv + 1,)), dma(()), dma((n - 1,)), dma(()), dma((n, n)), dma((n, n)), dma((2,)), dma((2,)), dma((2,)),
            dma((n, 2)), dma((n, 2)), dma((n, 2)),
            dma((count,)), dma((count,)), dma((count,)), dma((count,)),
            dma((n, 2, kv)), dma((n, 2, kv)),
            dma((2 * n,)), dma((2 * n,)), dma((2 * n,)), dma((2 * n,)),
            dma((2 * n,)), dma((2, n)),
            dma((2, n - 1)), dma((2, n)),
        ],
        compiler_params=pltpu.CompilerParams(
            collective_id=0, has_side_effects=True, vmem_limit_bytes=VMEM_LIMIT
        ),
    )(tokens, gain, post_gain, cosine, sine, w_query, w_key, w_value, w_out)


def tables(rows):
    half = HEAD_DIM // 2
    freq = np.float32(rope_base) ** (-(np.arange(half, dtype=np.float32) * np.float32(2.0 / HEAD_DIM)))
    angle = np.arange(rows, dtype=np.float32)[:, None] * freq[None, :].astype(np.float32)
    cosine, sine = np.cos(angle), np.sin(angle)
    return (
        jnp.asarray(np.concatenate([cosine, cosine], axis=1), jnp.float32),
        jnp.asarray(np.concatenate([-sine, sine], axis=1), jnp.float32),
    )


def solution(mesh):
    n_fsdp, n_tensor = mesh.shape["fsdp"], mesh.shape["tensor"]

    def on_device(tokens, norm_gain, w_query, w_key, w_value, w_out, post_gain):
        rows = tokens.shape[0]
        width = tokens.shape[1] * n_tensor
        if n_fsdp == n_tensor == CHAIN:
            return whole_block(
                n_fsdp, tokens, norm_gain, post_gain, *tables(rows), w_query, w_key, w_value, w_out
            )
        widened = tokens.astype(jnp.float32)
        total = lax.psum(jnp.sum(widened * widened, axis=1), "tensor")
        normed = (
            widened * lax.rsqrt(total / width + eps_norm)[:, None] * norm_gain.astype(jnp.float32)
        ).astype(jnp.bfloat16)
        mine = to_rows(normed, n_fsdp, n_tensor)
        raw = []
        for piece in (w_query, w_key, w_value):
            part = jnp.dot(mine, piece, preferred_element_type=jnp.float32).astype(jnp.bfloat16)
            parts = lax.all_to_all(part, "fsdp", 0, 0, tiled=True)
            parts = parts.reshape(n_fsdp, rows, piece.shape[1])
            raw.append(jnp.sum(parts.astype(jnp.float32), axis=0))
        query_raw, key_raw, value_raw = raw
        position = jnp.arange(rows, dtype=jnp.int32)
        local_heads = w_query.shape[1] // HEAD_DIM
        local_kv = w_key.shape[1] // HEAD_DIM
        query = rotate(query_raw.reshape(rows, local_heads, HEAD_DIM), position)
        key = rotate(key_raw.reshape(rows, local_kv, HEAD_DIM), position)
        query, key = query.astype(jnp.bfloat16), key.astype(jnp.bfloat16)
        value = value_raw.astype(jnp.bfloat16).reshape(rows, local_kv, HEAD_DIM)
        attn = attend(query, key, value, position)
        attn_all = lax.all_gather(attn, "fsdp", axis=0, tiled=True)
        part = jnp.dot(attn_all, w_out, preferred_element_type=jnp.float32).astype(jnp.bfloat16)
        summed = lax.psum_scatter(part, "tensor", scatter_dimension=0, tiled=True)
        proj = from_rows(summed, rows, n_fsdp, n_tensor).astype(jnp.float32)
        post_total = lax.psum(jnp.sum(proj * proj, axis=1), "tensor")
        branch = (
            proj
            * lax.rsqrt(post_total / width + eps_norm)[:, None]
            * post_gain.astype(jnp.float32)
        )
        return tokens.astype(jnp.float32) + branch

    placed = (
        P(("groups", "fsdp"), "tensor"),
        P("tensor"),
        P("fsdp", "tensor"),
        P("fsdp", "tensor"),
        P("fsdp", "tensor"),
        P("tensor", "fsdp"),
        P("tensor"),
    )
    return jax.shard_map(
        on_device,
        mesh=mesh,
        in_specs=placed,
        out_specs=P(("groups", "fsdp"), "tensor"),
        check_vma=False,
    )
```
